128 devices in a mesh: dp: 128 (over x, z, y, core).
Axes of the slice: x: 4, y: 4, z: 4, core: 2. Of those that a mesh axis runs over, the one named last changes fastest.
Arguments:
- gradients: bfloat16 [128, 256, 5120], P('dp'), may hold values from -6 to 6
- momentum: bfloat16 [256, 5120], replicated, may hold values from -6 to 6
- worker_error: bfloat16 [128, 256, 5120], P('dp'), may hold values from -1.796875 to 1.796875
- server_error: bfloat16 [256, 5120], P('dp'), may hold values from -1.796875 to 1.796875
- params: float32 [256, 5120], replicated, may hold values from -6 to 6
- variance: bfloat16 [256, 5120], replicated, may hold values from 0.099609375 to 4
Outputs:
- params_next: float32 [256, 5120], replicated
- momentum_next: bfloat16 [256, 5120], replicated
- worker_next: bfloat16 [128, 256, 5120], P('dp')
- server_next: bfloat16 [256, 5120], P('dp')
The draws below stay inside these ranges and needn't reach their ends.
All inputs are finite; a program needn't handle non-finite values.
Results may differ from the reference program's by a relative error of at most 0.0082.
Values may be sent and summed in bfloat16 or wider, within the bound.
A program may use at most 128 MiB of HBM per device.

```python
import math
import jax
import jax.numpy as jnp
from jax import lax

D = 5120
ROW_DEV = 2
ROWS = 256
N_DP = 128


def level_of(rng, dims, cuts, low, largest):
    gain = 1.0
    for position, blocks in cuts:
        heights = jax.random.uniform(jax.random.fold_in(jax.random.fold_in(rng, 6), position), (blocks,), jnp.float32, low / len(cuts), largest / len(cuts))
        gain = gain * jnp.repeat(jnp.exp(heights), dims[position] // blocks).reshape((-1,) + (1,) * (len(dims) - 1 - position))
    return gain


def centred(own_key, shape, spread, limit, cuts=(), dtype=jnp.bfloat16):
    result = jax.random.normal(own_key, shape, jnp.float32) * spread
    if len(cuts) > 0:
        result = level_of(own_key, shape, cuts, -0.22, 0.18) * result
    return jnp.clip(result, min=-limit, max=limit).astype(dtype)


def setup_inputs(seed: int = 0) -> dict:
    keys = jax.random.split(jax.random.key(seed), 7)
    return {
        "gradients": centred(keys[0], (N_DP, ROWS, D), 1.0, 6.0, ((0, 128),)),
        "momentum": centred(keys[1], (ROWS, D), 1.0, 6.0),
        "worker_error": centred(keys[2], (N_DP, ROWS, D), 0.3, 1.796875, ((0, 128),)),
        "server_error": centred(keys[3], (ROWS, D), 0.3, 1.796875, ((0, 128),)),
        "params": centred(keys[4], (ROWS, D), 1.0, 6.0, (), jnp.float32),
        "variance": jnp.clip(jnp.exp(jax.random.uniform(keys[5], (ROWS, D), jnp.float32, math.log(0.099609375), math.log(4.0))), 0.099609375, 4.0).astype(jnp.bfloat16),
    }


def to_scale(blocks):
    rounded = jnp.sqrt(lax.optimization_barrier(jnp.mean(blocks * blocks, axis=1))).astype(jnp.bfloat16)
    rounded = lax.optimization_barrier(rounded)
    return rounded.astype(jnp.float32)

def reference(gradients, momentum, worker_error, server_error, params, variance):
    moment = momentum.astype(jnp.float32)

    def replica(summed, pieces):
        grad_piece, error_piece = pieces
        combined = 0.875 * moment + 0.125 * grad_piece.astype(jnp.float32) + error_piece.astype(jnp.float32)
        blocks = combined.reshape(N_DP, ROW_DEV * D)
        group_scale = to_scale(blocks)
        compressed = jnp.where(blocks >= 0, 1.0, -1.0).astype(jnp.float32) * group_scale[:, None]
        worker_next = (blocks - compressed).reshape(ROWS, D).astype(jnp.bfloat16)
        return (summed + compressed, worker_next)
    start = jnp.zeros((N_DP, ROW_DEV * D), jnp.float32)
    summed, worker_next = lax.scan(replica, start, (gradients, worker_error))
    averaged = summed / N_DP
    served = averaged + server_error.astype(jnp.float32).reshape(N_DP, ROW_DEV * D)
    server_scale = to_scale(served)
    compressed = jnp.where(served >= 0, 1.0, -1.0).astype(jnp.float32) * server_scale[:, None]
    momentum_next = compressed.reshape(ROWS, D).astype(jnp.bfloat16)
    server_next = (served - compressed).reshape(ROWS, D).astype(jnp.bfloat16)
    denom = jnp.sqrt(variance.astype(jnp.float32)) + 1e-08
    params_next = params - 0.5 * momentum_next.astype(jnp.float32) / denom
    return (params_next, momentum_next, worker_next, server_next)
```

```python
import jax
import jax.numpy as jnp
from jax import lax
from jax.experimental import pallas as pl
from jax.experimental.pallas import tpu as pltpu
from jax.sharding import Mesh
from jax.sharding import PartitionSpec as P

MESH = pl.DeviceIdType.MESH
F32, BF16 = jnp.float32, jnp.bfloat16
DP = ("dp_0", "dp_1", "dp_2", "dp_3")
ORDERS = ((0, 1, 2), (1, 2, 0), (2, 0, 1))
ROWS, COLS, N_DEV = 256, 5120, 128
LANES = 128
W = 7 * LANES
WIDTHS = (W, W, W, W, W, COLS - 5 * W)
N_BLOCK = (ROWS // N_DEV) * COLS
N_SEND = 132


def lane_tile(start):
    return pl.ds(pl.multiple_of(start, LANES), LANES)


def swap_granules(tiles):
    low = lax.broadcasted_iota(jnp.int32, (8, LANES), 0) < 4
    swapped = []
    for i in range(4):
        pairs = []
        for first, second in ((tiles[0], tiles[1]), (tiles[2], tiles[3])):
            a, b = first[i // 2], second[i // 2]
            if i % 2 == 0:
                pairs.append(jnp.where(low, a, pltpu.roll(b, 4, 0)))
            else:
                pairs.append(jnp.where(low, pltpu.roll(a, 4, 0), b))
        swapped.append(pairs)
    return swapped


def compress_kernel(g_hbm, m_hbm, e_hbm, w_hbm, o_ref, g, m, e, comb, scale, w, in_sem, out_sem):
    chunk = 32
    loads = []
    for i in range(ROWS // chunk):
        rows = pl.ds(i * chunk, chunk)
        group = []
        for n, (src, dst) in enumerate(((g_hbm, g), (m_hbm, m), (e_hbm, e))):
            copy = pltpu.make_async_copy(src.at[rows], dst.at[rows], in_sem.at[n, i])
            copy.start()
            group.append(copy)
        loads.append(group)

    even = lax.broadcasted_iota(jnp.int32, (8, LANES), 0) % 2 == 0
    for i in range(ROWS // chunk):
        for copy in loads[i]:
            copy.wait()
        rows = pl.ds(i * chunk, chunk)

        def square(t, acc):
            cols = lane_tile(t * LANES)
            value = (
                0.875 * m[rows, cols].astype(F32)
                + 0.125 * g[rows, cols].astype(F32)
                + e[rows, cols].astype(F32)
            )
            comb[rows, cols] = value
            return acc + value * value

        acc = lax.fori_loop(0, COLS // LANES, square, jnp.zeros((chunk, LANES), F32), unroll=4)
        for s in range(chunk // 8):
            row = jnp.sum(acc[8 * s : 8 * s + 8], axis=1, keepdims=True)
            row = jnp.broadcast_to(row, (8, LANES))
            both = row + jnp.where(even, pltpu.roll(row, 7, 0), pltpu.roll(row, 1, 0))
            rounded = jnp.sqrt(both * (1.0 / N_BLOCK)).astype(BF16)
            scale[pl.ds(i * chunk + 8 * s, 8)] = rounded.astype(F32)

    stores = []
    for piece in range(6):
        k, h = divmod(piece, 2)

        def column(j, carry, piece=piece, k=k, h=h):
            src, dst = lane_tile(piece * W + j * LANES), lane_tile(j * LANES)
            for outer in range(4):
                tiles = []
                for inner in range(4):
                    x, z = (inner, outer) if k == 1 else (outer, inner)
                    top = 16 * (4 * x + z)
                    parts, rests = [], []
                    for s in range(2):
                        rows = pl.ds(top + 8 * s, 8)
                        value, size = comb[rows, src], scale[rows]
                        part = jnp.where(value >= 0, size, -size)
                        parts.append(part)
                        rests.append(value - part)
                    w[pl.ds(top, 16), src] = jnp.concatenate(rests, 0).astype(BF16)
                    tiles.append(parts)
                if k != 0:
                    tiles = swap_granules(tiles)
                for i in range(4):
                    far, near = (i, outer) if k == 2 else (outer, i)
                    half, row = 2 * far + near // 2, (near % 2) * 16
                    o_ref[k, h, half, pl.ds(row, 16), dst] = jnp.concatenate(tiles[i], 0).astype(BF16)
            return carry

        lax.fori_loop(0, WIDTHS[piece] // LANES, column, 0)
        if WIDTHS[piece] < W:
            rest = W - WIDTHS[piece]
            for half in range(8):
                o_ref[k, h, half, :, pl.ds(WIDTHS[piece], rest)] = jnp.zeros((32, rest), BF16)
        cols = pl.ds(piece * W, WIDTHS[piece])
        copy = pltpu.make_async_copy(w.at[:, cols], w_hbm.at[:, cols], out_sem.at[piece])
        copy.start()
        stores.append(copy)
    for copy in stores:
        copy.wait()


def exchange_kernel(
    o, se, m, sn,
    ra, rd, ro, rb1, rb2, sb2, s1, r2, st, s2, r3, sv, mb, rq,
    send_sem, ra_sem, rd_sem, rb1_sem, rb2_sem, r2_sem, r3_sem, rq_sem, q2_sem, q3_sem, d_sem,
):
    pos = [lax.axis_index(DP[a]) for a in range(3)]
    c = lax.axis_index(DP[3])
    other = 1 - c

    def step(v, d):
        return lax.rem(v + d, 4)

    def device(axis, delta, core):
        at = list(pos)
        if delta:
            at[axis] = step(pos[axis], delta)
        return (*at, core)

    sent = []

    def push(src, dst, sem, to):
        copy = pltpu.make_async_remote_copy(
            src_ref=src, dst_ref=dst, send_sem=send_sem.at[len(sent)], recv_sem=sem,
            device_id=to, device_id_type=MESH,
        )
        copy.start()
        sent.append(copy)

    def arrived(dst, sem):
        pltpu.make_async_remote_copy(
            src_ref=dst, dst_ref=dst, send_sem=send_sem.at[0], recv_sem=sem,
            device_id=device(0, 0, other), device_id_type=MESH,
        ).wait_recv()

    barrier = pltpu.get_barrier_semaphore()
    peers = [device(0, 0, other)]
    for axis in range(3):
        for delta in (1, 3, 2):
            for core in range(2):
                peers.append(device(axis, delta, core))
    for peer in peers:
        pl.semaphore_signal(barrier, inc=1, device_id=peer, device_id_type=MESH)
    pl.semaphore_wait(barrier, len(peers))

    partner = device(0, 0, other)
    ring = [tuple(step(pos[order[0]], d) for d in range(4)) for order in ORDERS]

    for k, order in enumerate(ORDERS):
        p2 = ring[k][2]
        for h in range(2):
            push(o.at[k, h, 2 * p2], ra.at[k, 0, c], ra_sem.at[k, 0, c], device(order[0], 1, h))
            push(o.at[k, h, 2 * p2 + 1], ra.at[k, 1, c], ra_sem.at[k, 1, c], device(order[0], 3, h))
    for k, order in enumerate(ORDERS):
        p, p1, _, p3 = ring[k]
        push(o.at[k, other, 2 * p1], rd.at[k, 0], rd_sem.at[k, 0], partner)
        push(o.at[k, other, 2 * p3 + 1], rd.at[k, 1], rd_sem.at[k, 1], partner)
    for k, order in enumerate(ORDERS):
        p, p1, _, p3 = ring[k]
        for h in range(2):
            push(o.at[k, h, 2 * p1 + 1], rb1.at[k, 0, c], rb1_sem.at[k, 0, c], device(order[0], 1, h))
            push(o.at[k, h, 2 * p3], rb1.at[k, 1, c], rb1_sem.at[k, 1, c], device(order[0], 3, h))
    for k in range(3):
        push(o.at[k, other, pl.ds(2 * ring[k][0], 2)], ro.at[k], rd_sem.at[k, 2], partner)
    for k, order in enumerate(ORDERS):
        p, p1, _, p3 = ring[k]
        for d in range(2):
            arrived(rd.at[k, d], rd_sem.at[k, d])
            for core in range(2):
                arrived(ra.at[k, d, core], ra_sem.at[k, d, core])
            for half in range(2):
                rows = pl.ds(16 * half, 16)
                sb2[k, d, rows] = (
                    (o[k, c, 2 * p1 if d == 0 else 2 * p3 + 1, rows].astype(F32) + rd[k, d, rows].astype(F32))
                    + (ra[k, d, 0, rows].astype(F32) + ra[k, d, 1, rows].astype(F32))
                )
            push(sb2.at[k, d], rb2.at[k, d], rb2_sem.at[k, d], device(order[0], 1 if d == 0 else 3, c))

    for k, order in enumerate(ORDERS):
        p, q = ring[k][0], pos[order[1]]
        arrived(ro.at[k], rd_sem.at[k, 2])
        for d in range(2):
            for core in range(2):
                arrived(rb1.at[k, d, core], rb1_sem.at[k, d, core])
        for d in range(2):
            arrived(rb2.at[k, d], rb2_sem.at[k, d])
            for half in range(2):
                rows = pl.ds(16 * half, 16)
                s1[k, 2 * d + half] = (
                    (o[k, c, 2 * p + d, rows].astype(F32) + ro[k, d, rows].astype(F32))
                    + (rb1[k, 1 - d, 0, rows].astype(F32) + rb1[k, 1 - d, 1, rows].astype(F32))
                    + rb2[k, d, rows]
                )
        for delta in (2, 1, 3):
            push(
                s1.at[k, step(q, delta)], r2.at[k, delta - 1], r2_sem.at[k, delta - 1], device(order[1], delta, c)
            )

    for k, order in enumerate(ORDERS):
        q, r = pos[order[1]], pos[order[2]]
        for delta in range(1, 4):
            arrived(r2.at[k, delta - 1], r2_sem.at[k, delta - 1])
        st[k] = (s1[k, q] + r2[k, 0]) + (r2[k, 1] + r2[k, 2])
        for i in range(8):
            s2[k, i] = st[k, pl.ds(2 * i, 2), :]
        for delta in (2, 1, 3):
            for core in range(2):
                push(
                    s2.at[k, 2 * step(r, delta) + core], r3.at[k, delta, c], r3_sem.at[k, delta, c],
                    device(order[2], delta, core),
                )
        push(s2.at[k, 2 * r + other], r3.at[k, 0, c], r3_sem.at[k, 0, c], partner)
        r3[k, 0, c] = s2[k, 2 * r + c]

    squares = jnp.zeros((2, LANES), F32)
    for piece in range(6):
        k, h = divmod(piece, 2)
        if h == 0:
            arrived(r3.at[k, 0, other], r3_sem.at[k, 0, other])
            for delta in range(1, 4):
                for core in range(2):
                    arrived(r3.at[k, delta, core], r3_sem.at[k, delta, core])
        width = WIDTHS[piece]
        cols = pl.ds(0, width)
        total = (r3[k, 0, h, :, cols] + r3[k, 1, h, :, cols]) + (r3[k, 2, h, :, cols] + r3[k, 3, h, :, cols])
        served = total * (1.0 / N_DEV) + se[:, pl.ds(piece * W, width)].astype(F32)
        sv[piece, :, cols] = served
        for t in range(width // LANES):
            part = served[:, t * LANES : (t + 1) * LANES]
            squares = squares + part * part
    total = jnp.sum(jnp.sum(squares, axis=1, keepdims=True), axis=0, keepdims=True)
    size = jnp.sqrt(total * (1.0 / N_BLOCK)).astype(BF16).astype(F32)
    for piece in range(6):
        k, h = divmod(piece, 2)
        width = WIDTHS[piece]
        cols = pl.ds(0, width)
        served = sv[piece, :, cols]
        level = jnp.broadcast_to(size, (2, width))
        comp = jnp.where(served >= 0, level, -level)
        sn[:, pl.ds(piece * W, width)] = (served - comp).astype(BF16)
        mb[k, h, :, cols] = comp.astype(BF16)
        if width < W:
            mb[k, h, :, pl.ds(width, W - width)] = jnp.zeros((2, W - width), BF16)

    for k, order in enumerate(ORDERS):
        r = pos[order[2]]
        mine = 2 * r + c
        for delta in (2, 1, 3):
            for h in range(2):
                push(mb.at[k, h], rq.at[k, mine], rq_sem.at[k, mine], device(order[2], delta, h))
        push(mb.at[k, other], rq.at[k, mine], rq_sem.at[k, mine], partner)
        rq[k, mine] = mb[k, c]
    for k, order in enumerate(ORDERS):
        p, q, r = (pos[a] for a in order)
        arrived(rq.at[k, 2 * r + other], rq_sem.at[k, 2 * r + other])
        for delta in range(1, 4):
            for core in range(2):
                at = 2 * step(r, delta) + core
                arrived(rq.at[k, at], rq_sem.at[k, at])
        for i in range(8):
            st[k, pl.ds(2 * i, 2), :] = rq[k, i].astype(F32)
        m[k, c, p, q] = st[k].astype(BF16)
        for delta in (2, 1, 3):
            push(m.at[k, c, p, q], m.at[k, c, p, q], q2_sem.at[k, q], device(order[1], delta, c))
    for k, order in enumerate(ORDERS):
        p, q = pos[order[0]], pos[order[1]]
        for delta in range(1, 4):
            at = step(q, delta)
            arrived(m.at[k, c, p, at], q2_sem.at[k, at])
        for d in range(2):
            for half in (d, 1 - d):
                view = m.at[k, c, p, pl.ds(2 * half, 2)]
                push(view, view, q3_sem.at[k, d, half], device(order[0], 1 if d == 0 else 3, c))
        push(m.at[k, c, p], m.at[k, c, p], d_sem.at[k, 0], partner)
    for k, order in enumerate(ORDERS):
        _, p1, _, p3 = ring[k]
        for d in range(2):
            view = m.at[k, c, p3 if d == 0 else p1, pl.ds(2 * d, 2)]
            arrived(view, q3_sem.at[k, d, d])
            push(view, view, q3_sem.at[k, d, 2], device(order[0], 1 if d == 0 else 3, c))
    for k in range(3):
        _, p1, _, p3 = ring[k]
        for d in range(2):
            at = p3 if d == 0 else p1
            arrived(m.at[k, c, at, pl.ds(2 * (1 - d), 2)], q3_sem.at[k, d, 1 - d])
            push(m.at[k, c, at], m.at[k, c, at], d_sem.at[k, 1 + d], partner)
    for k in range(3):
        p2 = ring[k][2]
        for d in range(2):
            view = m.at[k, c, p2, pl.ds(2 * d, 2)]
            arrived(view, q3_sem.at[k, d, 2])
            push(view, view, d_sem.at[k, 3 + d], partner)
    for k in range(3):
        p, p1, p2, p3 = ring[k]
        for n, at in enumerate((p, p3, p1)):
            arrived(m.at[k, other, at], d_sem.at[k, n])
        for d in range(2):
            arrived(m.at[k, other, p2, pl.ds(2 * d, 2)], d_sem.at[k, 3 + d])
    for copy in sent:
        copy.wait_send()


def update_kernel(m, params, variance, params_next, momentum_next):
    piece = pl.program_id(0)

    for k in range(3):

        @pl.when(piece // 2 == k)
        def _(k=k):
            def column(j, carry):
                cols = lane_tile(j * LANES)
                for outer in range(4):
                    tiles = []
                    for i in range(4):
                        far, near = (i, outer) if k == 2 else (outer, i)
                        tile = m[0, 0, far, near, :, cols].astype(F32)
                        tiles.append([tile[:8], tile[8:]])
                    if k != 0:
                        tiles = swap_granules(tiles)
                    for inner in range(4):
                        x, z = (inner, outer) if k == 1 else (outer, inner)
                        rows = pl.ds(16 * (4 * x + z), 16)
                        value = jnp.concatenate(tiles[inner], 0)
                        momentum_next[rows, cols] = value.astype(BF16)
                        denom = jnp.sqrt(variance[rows, cols].astype(F32)) + 1e-08
                        params_next[rows, cols] = params[rows, cols] - 0.5 * value / denom
                return carry

            lax.fori_loop(0, W // LANES, column, 0)


def local(gradients, momentum, worker_error, server_error, params, variance):
    hbm = pl.BlockSpec(memory_space=pl.ANY)
    vmem = pl.BlockSpec(memory_space=pltpu.VMEM)
    worker_next, outgoing = pl.pallas_call(
        compress_kernel,
        out_shape=(
            jax.ShapeDtypeStruct((ROWS, COLS), BF16),
            jax.ShapeDtypeStruct((3, 2, 8, 32, W), BF16),
        ),
        in_specs=[hbm] * 3,
        out_specs=(hbm, vmem),
        scratch_shapes=[
            pltpu.VMEM((ROWS, COLS), BF16),
            pltpu.VMEM((ROWS, COLS), BF16),
            pltpu.VMEM((ROWS, COLS), BF16),
            pltpu.VMEM((ROWS, COLS), F32),
            pltpu.VMEM((ROWS, LANES), F32),
            pltpu.VMEM((ROWS, COLS), BF16),
            pltpu.SemaphoreType.DMA((3, 8)),
            pltpu.SemaphoreType.DMA((6,)),
        ],
        compiler_params=pltpu.CompilerParams(vmem_limit_bytes=26 * 2**20),
        name="compress",
    )(gradients.reshape(ROWS, COLS), momentum, worker_error.reshape(ROWS, COLS))

    dma = pltpu.SemaphoreType.DMA
    gathered, server_next = pl.pallas_call(
        exchange_kernel,
        out_shape=(
            jax.ShapeDtypeStruct((3, 2, 4, 4, 16, W), BF16),
            jax.ShapeDtypeStruct((2, COLS), BF16),
        ),
        in_specs=[vmem, vmem],
        out_specs=(vmem, vmem),
        scratch_shapes=[
            pltpu.VMEM((3, 2, 2, 32, W), BF16),
            pltpu.VMEM((3, 2, 32, W), BF16),
            pltpu.VMEM((3, 2, 32, W), BF16),
            pltpu.VMEM((3, 2, 2, 32, W), BF16),
            pltpu.VMEM((3, 2, 32, W), F32),
            pltpu.VMEM((3, 2, 32, W), F32),
            pltpu.VMEM((3, 4, 16, W), F32),
            pltpu.VMEM((3, 3, 16, W), F32),
            pltpu.VMEM((3, 16, W), F32),
            pltpu.VMEM((3, 8, 2, W), F32),
            pltpu.VMEM((3, 4, 2, 2, W), F32),
            pltpu.VMEM((6, 2, W), F32),
            pltpu.VMEM((3, 2, 2, W), BF16),
            pltpu.VMEM((3, 8, 2, W), BF16),
            dma((N_SEND,)),
            dma((3, 2, 2)),
            dma((3, 3)),
            dma((3, 2, 2)),
            dma((3, 2)),
            dma((3, 3)),
            dma((3, 4, 2)),
            dma((3, 8)),
            dma((3, 4)),
            dma((3, 2, 3)),
            dma((3, 5)),
        ],
        compiler_params=pltpu.CompilerParams(
            collective_id=0, has_side_effects=True, vmem_limit_bytes=20 * 2**20
        ),
        name="exchange",
    )(outgoing, server_error)

    params_next, momentum_next = pl.pallas_call(
        update_kernel,
        grid=(6,),
        out_shape=(
            jax.ShapeDtypeStruct((ROWS, COLS), F32),
            jax.ShapeDtypeStruct((ROWS, COLS), BF16),
        ),
        in_specs=[
            pl.BlockSpec((1, 1, 4, 4, 16, W), lambda i: (i // 2, i % 2, 0, 0, 0, 0)),
            pl.BlockSpec((ROWS, W), lambda i: (0, i)),
            pl.BlockSpec((ROWS, W), lambda i: (0, i)),
        ],
        out_specs=(
            pl.BlockSpec((ROWS, W), lambda i: (0, i)),
            pl.BlockSpec((ROWS, W), lambda i: (0, i)),
        ),
        compiler_params=pltpu.CompilerParams(vmem_limit_bytes=16 * 2**20),
        name="update",
    )(gathered, params, variance)
    return (params_next, momentum_next, worker_next.reshape(1, ROWS, COLS), server_next)


def solution(mesh):
    split = Mesh(mesh.devices.reshape(4, 4, 4, 2), DP)
    in_specs = (P(DP, None, None), P(), P(DP, None, None), P(DP, None), P(), P())
    out_specs = (P(), P(), P(DP, None, None), P(DP, None))
    return jax.shard_map(local, mesh=split, in_specs=in_specs, out_specs=out_specs, check_vma=False)
```

```python
import jax
import jax.numpy as jnp
from jax import lax
from jax.experimental import pallas as pl
from jax.experimental.pallas import tpu as pltpu
from jax.sharding import Mesh
from jax.sharding import PartitionSpec as P

MESH = pl.DeviceIdType.MESH
F32, BF16 = jnp.float32, jnp.bfloat16
DP = ("dp_0", "dp_1", "dp_2", "dp_3")
ORDERS = ((0, 1, 2), (1, 2, 0), (2, 0, 1))
ROWS, COLS, N_DEV = 256, 5120, 128
LANES = 128
W = 7 * LANES
WIDTHS = (W, W, W, W, W, COLS - 5 * W)
N_BLOCK = (ROWS // N_DEV) * COLS
N_SEND = 132
VMEM_STEP, VMEM_UPDATE = 26 * 2**20, 9 * 2**20


def lane_tile(start):
    return pl.ds(pl.multiple_of(start, LANES), LANES)


def swap_granules(tiles):
    low = lax.broadcasted_iota(jnp.int32, (8, LANES), 0) < 4
    swapped = []
    for i in range(4):
        pairs = []
        for first, second in ((tiles[0], tiles[1]), (tiles[2], tiles[3])):
            a, b = first[i // 2], second[i // 2]
            if i % 2 == 0:
                pairs.append(jnp.where(low, a, pltpu.roll(b, 4, 0)))
            else:
                pairs.append(jnp.where(low, pltpu.roll(a, 4, 0), b))
        swapped.append(pairs)
    return swapped


def step_kernel(
    g_hbm, m_hbm, e_hbm, se_hbm, p_hbm, v_hbm, m, sn, wn, rate, pv,
    gv, mv, ev, vv, se, comb, scale, o, ra, rd, ro, rb1, rb2, sb2, s1, r2, st, s2, r3, sv, mb, rq,
    in_sem, aux_sem,
    send_sem, ra_sem, rd_sem, rb1_sem, rb2_sem, r2_sem, r3_sem, rq_sem, q2_sem, q3_sem, d_sem,
):
    pos = [lax.axis_index(DP[a]) for a in range(3)]
    c = lax.axis_index(DP[3])
    other = 1 - c

    def step(v, d):
        return lax.rem(v + d, 4)

    def device(axis, delta, core):
        at = list(pos)
        if delta:
            at[axis] = step(pos[axis], delta)
        return (*at, core)

    sent = []

    def push(src, dst, sem, to):
        copy = pltpu.make_async_remote_copy(
            src_ref=src, dst_ref=dst, send_sem=send_sem.at[len(sent)], recv_sem=sem,
            device_id=to, device_id_type=MESH,
        )
        copy.start()
        sent.append(copy)

    def arrived(dst, sem):
        pltpu.make_async_remote_copy(
            src_ref=dst, dst_ref=dst, send_sem=send_sem.at[0], recv_sem=sem,
            device_id=device(0, 0, other), device_id_type=MESH,
        ).wait_recv()

    barrier = pltpu.get_barrier_semaphore()
    peers = [device(0, 0, other)]
    for axis in range(3):
        for delta in (1, 3, 2):
            for core in range(2):
                peers.append(device(axis, delta, core))
    for peer in peers:
        pl.semaphore_signal(barrier, inc=1, device_id=peer, device_id_type=MESH)

    chunk = 32
    loads = []
    for i in range(ROWS // chunk):
        rows = pl.ds(i * chunk, chunk)
        group = []
        for n, (src, dst) in enumerate(((g_hbm, gv), (m_hbm, mv), (e_hbm, ev))):
            copy = pltpu.make_async_copy(src.at[rows], dst.at[rows], in_sem.at[n, i])
            copy.start()
            group.append(copy)
        loads.append(group)

    even = lax.broadcasted_iota(jnp.int32, (8, LANES), 0) % 2 == 0
    for i in range(ROWS // chunk):
        for copy in loads[i]:
            copy.wait()
        rows = pl.ds(i * chunk, chunk)

        def square(t, acc, rows=rows):
            cols = lane_tile(t * LANES)
            value = (
                0.875 * mv[rows, cols].astype(F32)
                + 0.125 * gv[rows, cols].astype(F32)
                + ev[rows, cols].astype(F32)
            )
            comb[rows, cols] = value
            return acc + value * value

        acc = lax.fori_loop(0, COLS // LANES, square, jnp.zeros((chunk, LANES), F32), unroll=4)
        for s in range(chunk // 8):
            row = jnp.sum(acc[8 * s : 8 * s + 8], axis=1, keepdims=True)
            row = jnp.broadcast_to(row, (8, LANES))
            both = row + jnp.where(even, pltpu.roll(row, 7, 0), pltpu.roll(row, 1, 0))
            rounded = jnp.sqrt(both * (1.0 / N_BLOCK)).astype(BF16)
            scale[pl.ds(i * chunk + 8 * s, 8)] = rounded.astype(F32)

    se_copy = pltpu.make_async_copy(se_hbm, se, aux_sem.at[0])
    v_copy = pltpu.make_async_copy(v_hbm, vv, aux_sem.at[1])
    p_copy = pltpu.make_async_copy(p_hbm, pv, aux_sem.at[2])
    for copy in (se_copy, v_copy, p_copy):
        copy.start()
    pl.semaphore_wait(barrier, len(peers))

    partner = device(0, 0, other)
    ring = [tuple(step(pos[order[0]], d) for d in range(4)) for order in ORDERS]

    for h in range(2):
        for k, order in enumerate(ORDERS):
            piece = 2 * k + h

            def column(j, carry, piece=piece, k=k, h=h):
                src, dst = lane_tile(piece * W + j * LANES), lane_tile(j * LANES)
                for outer in range(4):
                    tiles = []
                    for inner in range(4):
                        x, z = (inner, outer) if k == 1 else (outer, inner)
                        parts = []
                        for s in range(2):
                            rows = pl.ds(16 * (4 * x + z) + 8 * s, 8)
                            size = scale[rows]
                            parts.append(jnp.where(comb[rows, src] >= 0, size, -size))
                        tiles.append(parts)
                    if k != 0:
                        tiles = swap_granules(tiles)
                    for i in range(4):
                        far, near = (i, outer) if k == 2 else (outer, i)
                        half, row = 2 * far + near // 2, (near % 2) * 16
                        o[k, h, half, pl.ds(row, 16), dst] = jnp.concatenate(tiles[i], 0).astype(BF16)
                return carry

            lax.fori_loop(0, WIDTHS[piece] // LANES, column, 0)
            if WIDTHS[piece] < W:
                spare = W - WIDTHS[piece]
                for half in range(8):
                    o[k, h, half, :, pl.ds(WIDTHS[piece], spare)] = jnp.zeros((32, spare), BF16)
            p2 = ring[k][2]
            push(o.at[k, h, 2 * p2], ra.at[k, 0, c], ra_sem.at[k, 0, c], device(order[0], 1, h))
            push(o.at[k, h, 2 * p2 + 1], ra.at[k, 1, c], ra_sem.at[k, 1, c], device(order[0], 3, h))
    for k, order in enumerate(ORDERS):
        p, p1, _, p3 = ring[k]
        push(o.at[k, other, 2 * p1], rd.at[k, 0], rd_sem.at[k, 0], partner)
        push(o.at[k, other, 2 * p3 + 1], rd.at[k, 1], rd_sem.at[k, 1], partner)
    for k, order in enumerate(ORDERS):
        p, p1, _, p3 = ring[k]
        for h in range(2):
            push(o.at[k, h, 2 * p1 + 1], rb1.at[k, 0, c], rb1_sem.at[k, 0, c], device(order[0], 1, h))
            push(o.at[k, h, 2 * p3], rb1.at[k, 1, c], rb1_sem.at[k, 1, c], device(order[0], 3, h))
    for k in range(3):
        push(o.at[k, other, pl.ds(2 * ring[k][0], 2)], ro.at[k], rd_sem.at[k, 2], partner)
    def rest_column(j, carry):
        cols = lane_tile(j * LANES)
        for top in range(0, ROWS, 16):
            rows = pl.ds(top, 16)
            value, size = comb[rows, cols], scale[rows]
            wn[rows, cols] = (value - jnp.where(value >= 0, size, -size)).astype(BF16)
        return carry

    lax.fori_loop(0, COLS // LANES, rest_column, 0)

    for k, order in enumerate(ORDERS):
        p, p1, _, p3 = ring[k]
        for d in range(2):
            arrived(rd.at[k, d], rd_sem.at[k, d])
            for core in range(2):
                arrived(ra.at[k, d, core], ra_sem.at[k, d, core])
            for half in range(2):
                rows = pl.ds(16 * half, 16)
                sb2[k, d, rows] = (
                    (o[k, c, 2 * p1 if d == 0 else 2 * p3 + 1, rows].astype(F32) + rd[k, d, rows].astype(F32))
                    + (ra[k, d, 0, rows].astype(F32) + ra[k, d, 1, rows].astype(F32))
                )
            push(sb2.at[k, d], rb2.at[k, d], rb2_sem.at[k, d], device(order[0], 1 if d == 0 else 3, c))

    for k, order in enumerate(ORDERS):
        p, q = ring[k][0], pos[order[1]]
        arrived(ro.at[k], rd_sem.at[k, 2])
        for d in range(2):
            for core in range(2):
                arrived(rb1.at[k, d, core], rb1_sem.at[k, d, core])
        for d in range(2):
            arrived(rb2.at[k, d], rb2_sem.at[k, d])
            for half in range(2):
                rows = pl.ds(16 * half, 16)
                s1[k, 2 * d + half] = (
                    (o[k, c, 2 * p + d, rows].astype(F32) + ro[k, d, rows].astype(F32))
                    + (rb1[k, 1 - d, 0, rows].astype(F32) + rb1[k, 1 - d, 1, rows].astype(F32))
                    + rb2[k, d, rows]
                )
        for delta in (2, 1, 3):
            push(
                s1.at[k, step(q, delta)], r2.at[k, delta - 1], r2_sem.at[k, delta - 1], device(order[1], delta, c)
            )

    def rate_column(j, carry):
        cols = lane_tile(j * LANES)
        for top in range(0, ROWS, 16):
            rows = pl.ds(top, 16)
            rate[rows, cols] = 0.5 / (jnp.sqrt(vv[rows, cols].astype(F32)) + 1e-08)
        return carry

    v_copy.wait()
    lax.fori_loop(0, COLS // LANES, rate_column, 0)

    for k, order in enumerate(ORDERS):
        q, r = pos[order[1]], pos[order[2]]
        for delta in range(1, 4):
            arrived(r2.at[k, delta - 1], r2_sem.at[k, delta - 1])
        st[k] = (s1[k, q] + r2[k, 0]) + (r2[k, 1] + r2[k, 2])
        for i in range(8):
            s2[k, i] = st[k, pl.ds(2 * i, 2), :]
        for delta in (2, 1, 3):
            for core in range(2):
                push(
                    s2.at[k, 2 * step(r, delta) + core], r3.at[k, delta, c], r3_sem.at[k, delta, c],
                    device(order[2], delta, core),
                )
        push(s2.at[k, 2 * r + other], r3.at[k, 0, c], r3_sem.at[k, 0, c], partner)
        r3[k, 0, c] = s2[k, 2 * r + c]

    se_copy.wait()
    squares = jnp.zeros((2, LANES), F32)
    for piece in range(6):
        k, h = divmod(piece, 2)
        if h == 0:
            arrived(r3.at[k, 0, other], r3_sem.at[k, 0, other])
            for delta in range(1, 4):
                for core in range(2):
                    arrived(r3.at[k, delta, core], r3_sem.at[k, delta, core])
        width = WIDTHS[piece]
        cols = pl.ds(0, width)
        total = (r3[k, 0, h, :, cols] + r3[k, 1, h, :, cols]) + (r3[k, 2, h, :, cols] + r3[k, 3, h, :, cols])
        served = total * (1.0 / N_DEV) + se[:, pl.ds(piece * W, width)].astype(F32)
        sv[piece, :, cols] = served
        for t in range(width // LANES):
            part = served[:, t * LANES : (t + 1) * LANES]
            squares = squares + part * part
    total = jnp.sum(jnp.sum(squares, axis=1, keepdims=True), axis=0, keepdims=True)
    size = jnp.sqrt(total * (1.0 / N_BLOCK)).astype(BF16).astype(F32)
    for piece in range(6):
        k, h = divmod(piece, 2)
        width = WIDTHS[piece]
        cols = pl.ds(0, width)
        served = sv[piece, :, cols]
        level = jnp.broadcast_to(size, (2, width))
        comp = jnp.where(served >= 0, level, -level)
        sn[:, pl.ds(piece * W, width)] = (served - comp).astype(BF16)
        mb[k, h, :, cols] = comp.astype(BF16)
        if width < W:
            mb[k, h, :, pl.ds(width, W - width)] = jnp.zeros((2, W - width), BF16)

    for k, order in enumerate(ORDERS):
        r = pos[order[2]]
        mine = 2 * r + c
        for delta in (2, 1, 3):
            for h in range(2):
                push(mb.at[k, h], rq.at[k, mine], rq_sem.at[k, mine], device(order[2], delta, h))
        push(mb.at[k, other], rq.at[k, mine], rq_sem.at[k, mine], partner)
        rq[k, mine] = mb[k, c]
    for k, order in enumerate(ORDERS):
        p, q, r = (pos[a] for a in order)
        arrived(rq.at[k, 2 * r + other], rq_sem.at[k, 2 * r + other])
        for delta in range(1, 4):
            for core in range(2):
                at = 2 * step(r, delta) + core
                arrived(rq.at[k, at], rq_sem.at[k, at])
        for i in range(8):
            st[k, pl.ds(2 * i, 2), :] = rq[k, i].astype(F32)
        m[k, c, p, q] = st[k].astype(BF16)
        for delta in (2, 1, 3):
            push(m.at[k, c, p, q], m.at[k, c, p, q], q2_sem.at[k, q], device(order[1], delta, c))
    for k, order in enumerate(ORDERS):
        p, q = pos[order[0]], pos[order[1]]
        for delta in range(1, 4):
            at = step(q, delta)
            arrived(m.at[k, c, p, at], q2_sem.at[k, at])
        for d in range(2):
            for half in (d, 1 - d):
                view = m.at[k, c, p, pl.ds(2 * half, 2)]
                push(view, view, q3_sem.at[k, d, half], device(order[0], 1 if d == 0 else 3, c))
        push(m.at[k, c, p], m.at[k, c, p], d_sem.at[k, 0], partner)
    for k, order in enumerate(ORDERS):
        _, p1, _, p3 = ring[k]
        for d in range(2):
            view = m.at[k, c, p3 if d == 0 else p1, pl.ds(2 * d, 2)]
            arrived(view, q3_sem.at[k, d, d])
            push(view, view, q3_sem.at[k, d, 2], device(order[0], 1 if d == 0 else 3, c))
    for k in range(3):
        _, p1, _, p3 = ring[k]
        for d in range(2):
            at = p3 if d == 0 else p1
            arrived(m.at[k, c, at, pl.ds(2 * (1 - d), 2)], q3_sem.at[k, d, 1 - d])
            push(m.at[k, c, at], m.at[k, c, at], d_sem.at[k, 1 + d], partner)
    for k in range(3):
        p2 = ring[k][2]
        for d in range(2):
            view = m.at[k, c, p2, pl.ds(2 * d, 2)]
            arrived(view, q3_sem.at[k, d, 2])
            push(view, view, d_sem.at[k, 3 + d], partner)
    for k in range(3):
        p, p1, p2, p3 = ring[k]
        for n, at in enumerate((p, p3, p1)):
            arrived(m.at[k, other, at], d_sem.at[k, n])
        for d in range(2):
            arrived(m.at[k, other, p2, pl.ds(2 * d, 2)], d_sem.at[k, 3 + d])
    p_copy.wait()
    for copy in sent:
        copy.wait_send()


def update_kernel(m, wn, sn, rate, pv, params_next, momentum_next, worker_next, server_next, pn, mn, sem):
    stores = [
        pltpu.make_async_copy(wn, worker_next, sem.at[0]),
        pltpu.make_async_copy(sn, server_next, sem.at[1]),
    ]
    for copy in stores:
        copy.start()
    for piece in range(6):
        k, h = divmod(piece, 2)

        def column(j, carry, piece=piece, k=k, h=h):
            src, dst = lane_tile(j * LANES), lane_tile(piece * W + j * LANES)
            for outer in range(4):
                tiles = []
                for i in range(4):
                    far, near = (i, outer) if k == 2 else (outer, i)
                    tile = m[k, h, far, near, :, src].astype(F32)
                    tiles.append([tile[:8], tile[8:]])
                if k != 0:
                    tiles = swap_granules(tiles)
                for inner in range(4):
                    x, z = (inner, outer) if k == 1 else (outer, inner)
                    rows = pl.ds(16 * (4 * x + z), 16)
                    value = jnp.concatenate(tiles[inner], 0)
                    mn[rows, dst] = value.astype(BF16)
                    pn[rows, dst] = pv[rows, dst] - value * rate[rows, dst]
            return carry

        lax.fori_loop(0, WIDTHS[piece] // LANES, column, 0)
        cols = pl.ds(piece * W, WIDTHS[piece])
        for n, (src, dst) in enumerate(((pn, params_next), (mn, momentum_next))):
            copy = pltpu.make_async_copy(src.at[:, cols], dst.at[:, cols], sem.at[2 + 2 * piece + n])
            copy.start()
            stores.append(copy)
    for copy in stores:
        copy.wait()


def local(gradients, momentum, worker_error, server_error, params, variance):
    hbm = pl.BlockSpec(memory_space=pltpu.HBM)
    vmem = pl.BlockSpec(memory_space=pltpu.VMEM)
    dma = pltpu.SemaphoreType.DMA
    whole = (ROWS, COLS)
    own = (ROWS // N_DEV, COLS)
    gathered, server_next, worker_next, rate, held = pl.pallas_call(
        step_kernel,
        out_shape=(
            pltpu.VMEM((3, 2, 4, 4, 16, W), BF16),
            pltpu.VMEM(own, BF16),
            pltpu.VMEM(whole, BF16),
            pltpu.VMEM(whole, F32),
            pltpu.VMEM(whole, F32),
        ),
        in_specs=[hbm] * 6,
        out_specs=(vmem,) * 5,
        scratch_shapes=[
            pltpu.VMEM(whole, BF16),
            pltpu.VMEM(whole, BF16),
            pltpu.VMEM(whole, BF16),
            pltpu.VMEM(whole, BF16),
            pltpu.VMEM(own, BF16),
            pltpu.VMEM(whole, F32),
            pltpu.VMEM((ROWS, LANES), F32),
            pltpu.VMEM((3, 2, 8, 32, W), BF16),
            pltpu.VMEM((3, 2, 2, 32, W), BF16),
            pltpu.VMEM((3, 2, 32, W), BF16),
            pltpu.VMEM((3, 2, 32, W), BF16),
            pltpu.VMEM((3, 2, 2, 32, W), BF16),
            pltpu.VMEM((3, 2, 32, W), F32),
            pltpu.VMEM((3, 2, 32, W), F32),
            pltpu.VMEM((3, 4, 16, W), F32),
            pltpu.VMEM((3, 3, 16, W), F32),
            pltpu.VMEM((3, 16, W), F32),
            pltpu.VMEM((3, 8, 2, W), F32),
            pltpu.VMEM((3, 4, 2, 2, W), F32),
            pltpu.VMEM((6, 2, W), F32),
            pltpu.VMEM((3, 2, 2, W), BF16),
            pltpu.VMEM((3, 8, 2, W), BF16),
            dma((3, 8)),
            dma((3,)),
            dma((N_SEND,)),
            dma((3, 2, 2)),
            dma((3, 3)),
            dma((3, 2, 2)),
            dma((3, 2)),
            dma((3, 3)),
            dma((3, 4, 2)),
            dma((3, 8)),
            dma((3, 4)),
            dma((3, 2, 3)),
            dma((3, 5)),
        ],
        compiler_params=pltpu.CompilerParams(
            collective_id=0, has_side_effects=True, vmem_limit_bytes=VMEM_STEP
        ),
        name="step",
    )(
        *(
            pltpu.with_memory_space_constraint(a, pltpu.HBM)
            for a in (
                gradients.reshape(whole), momentum, worker_error.reshape(whole), server_error, params, variance
            )
        )
    )

    params_next, momentum_next, worker_next, server_next = pl.pallas_call(
        update_kernel,
        out_shape=(
            jax.ShapeDtypeStruct(whole, F32),
            jax.ShapeDtypeStruct(whole, BF16),
            jax.ShapeDtypeStruct(whole, BF16),
            jax.ShapeDtypeStruct(own, BF16),
        ),
        in_specs=[vmem] * 5,
        out_specs=(hbm,) * 4,
        scratch_shapes=[pltpu.VMEM(whole, F32), pltpu.VMEM(whole, BF16), dma((14,))],
        compiler_params=pltpu.CompilerParams(vmem_limit_bytes=VMEM_UPDATE),
        name="update",
    )(
        *(
            pltpu.with_memory_space_constraint(a, pltpu.VMEM)
            for a in (gathered, worker_next, server_next, rate, held)
        )
    )
    return (params_next, momentum_next, worker_next.reshape(1, ROWS, COLS), server_next)


def solution(mesh):
    split = Mesh(mesh.devices.reshape(4, 4, 4, 2), DP)
    in_specs = (P(DP, None, None), P(), P(DP, None, None), P(DP, None), P(), P())
    out_specs = (P(), P(), P(DP, None, None), P(DP, None))
    return jax.shard_map(local, mesh=split, in_specs=in_specs, out_specs=out_specs, check_vma=False)
```

```python
import jax
import jax.numpy as jnp
from jax import lax
from jax.experimental import pallas as pl
from jax.experimental.pallas import tpu as pltpu
from jax.sharding import Mesh
from jax.sharding import PartitionSpec as P

MESH = pl.DeviceIdType.MESH
F32, BF16 = jnp.float32, jnp.bfloat16
DP = ("dp_0", "dp_1", "dp_2", "dp_3")
ORDERS = ((0, 1, 2), (1, 2, 0), (2, 0, 1))
ROWS, COLS, N_DEV = 256, 5120, 128
LANES = 128
W = 7 * LANES
WIDTHS = (W, W, W, W, W, COLS - 5 * W)
N_BLOCK = (ROWS // N_DEV) * COLS
CHUNK = 64
VMEM_STEP, VMEM_UPDATE = 26 * 2**20, 9 * 2**20


def lane_tile(start):
    return pl.ds(pl.multiple_of(start, LANES), LANES)


def swap_granules(tiles):
    low = lax.broadcasted_iota(jnp.int32, (8, LANES), 0) < 4
    swapped = []
    for i in range(4):
        pairs = []
        for first, second in ((tiles[0], tiles[1]), (tiles[2], tiles[3])):
            a, b = first[i // 2], second[i // 2]
            if i % 2 == 0:
                pairs.append(jnp.where(low, a, pltpu.roll(b, 4, 0)))
            else:
                pairs.append(jnp.where(low, pltpu.roll(a, 4, 0), b))
        swapped.append(pairs)
    return swapped


def step_kernel(
    g_hbm, m_hbm, e_hbm, se_hbm, p_hbm, v_hbm, m, sn, wn, rate, pv,
    gme, vv, se, comb, scale, o, ra, rb1, rb2, sb2, s1, r2, st, s2, r3, sv, mb, rq,
    in_sem, aux_sem, send_sem, ra_sem, rb1_sem, rb2_sem, r2_sem, r3_sem, rq_sem, q2_sem, q3_sem, d_sem,
):
    pos = [lax.axis_index(DP[a]) for a in range(3)]
    c = lax.axis_index(DP[3])
    other = 1 - c

    def step(v, d):
        return lax.rem(v + d, 4)

    def device(axis, delta, core):
        at = list(pos)
        if delta:
            at[axis] = step(pos[axis], delta)
        return (*at, core)

    def push(stage, src, dst, sem, to):
        pltpu.make_async_remote_copy(
            src_ref=src, dst_ref=dst, send_sem=send_sem.at[stage], recv_sem=sem,
            device_id=to, device_id_type=MESH,
        ).start()

    def left(stage, alike):
        pltpu.make_async_remote_copy(
            src_ref=alike, dst_ref=alike, send_sem=send_sem.at[stage], recv_sem=d_sem.at[0],
            device_id=device(0, 0, other), device_id_type=MESH,
        ).wait_send()

    def arrived(dst, sem):
        pltpu.make_async_remote_copy(
            src_ref=dst, dst_ref=dst, send_sem=send_sem.at[0], recv_sem=sem,
            device_id=device(0, 0, other), device_id_type=MESH,
        ).wait_recv()

    barrier = pltpu.get_barrier_semaphore()
    peers = [device(0, 0, other)]
    for axis in range(3):
        for delta in (1, 3, 2):
            for core in range(2):
                peers.append(device(axis, delta, core))
    for peer in peers:
        pl.semaphore_signal(barrier, inc=1, device_id=peer, device_id_type=MESH)

    for i in range(ROWS // CHUNK):
        rows = pl.ds(i * CHUNK, CHUNK)
        for n, src in enumerate((g_hbm, m_hbm, e_hbm)):
            pltpu.make_async_copy(src.at[rows], gme.at[n, rows], in_sem.at[i]).start()

    even = lax.broadcasted_iota(jnp.int32, (8, LANES), 0) % 2 == 0
    for i in range(ROWS // CHUNK):
        rows = pl.ds(i * CHUNK, CHUNK)
        pltpu.make_async_copy(gme.at[:, rows], gme.at[:, rows], in_sem.at[i]).wait()

        def square(t, acc, rows=rows):
            cols = lane_tile(t * LANES)
            value = (
                0.875 * gme[1, rows, cols].astype(F32)
                + 0.125 * gme[0, rows, cols].astype(F32)
                + gme[2, rows, cols].astype(F32)
            )
            comb[rows, cols] = value
            return acc + value * value

        acc = lax.fori_loop(0, COLS // LANES, square, jnp.zeros((CHUNK, LANES), F32), unroll=4)
        for s in range(CHUNK // 8):
            row = jnp.sum(acc[8 * s : 8 * s + 8], axis=1, keepdims=True)
            row = jnp.broadcast_to(row, (8, LANES))
            both = row + jnp.where(even, pltpu.roll(row, 7, 0), pltpu.roll(row, 1, 0))
            rounded = jnp.sqrt(both * (1.0 / N_BLOCK)).astype(BF16)
            scale[pl.ds(i * CHUNK + 8 * s, 8)] = rounded.astype(F32)

    se_copy = pltpu.make_async_copy(se_hbm, se, aux_sem.at[0])
    v_copy = pltpu.make_async_copy(v_hbm, vv, aux_sem.at[1])
    p_copy = pltpu.make_async_copy(p_hbm, pv, aux_sem.at[2])
    for copy in (se_copy, v_copy, p_copy):
        copy.start()
    pl.semaphore_wait(barrier, len(peers))

    partner = device(0, 0, other)
    ring = [tuple(step(pos[order[0]], d) for d in range(4)) for order in ORDERS]

    for h in range(2):
        for k, order in enumerate(ORDERS):
            piece = 2 * k + h

            def column(j, carry, piece=piece, k=k, h=h):
                src, dst = lane_tile(piece * W + j * LANES), lane_tile(j * LANES)
                for outer in range(4):
                    tiles = []
                    for inner in range(4):
                        x, z = (inner, outer) if k == 1 else (outer, inner)
                        parts = []
                        for s in range(2):
                            rows = pl.ds(16 * (4 * x + z) + 8 * s, 8)
                            size = scale[rows]
                            parts.append(jnp.where(comb[rows, src] >= 0, size, -size))
                        tiles.append(parts)
                    if k != 0:
                        tiles = swap_granules(tiles)
                    for i in range(4):
                        far, near = (i, outer) if k == 2 else (outer, i)
                        half, row = 2 * far + near // 2, (near % 2) * 16
                        o[k, h, half, pl.ds(row, 16), dst] = jnp.concatenate(tiles[i], 0).astype(BF16)
                return carry

            lax.fori_loop(0, WIDTHS[piece] // LANES, column, 0)
            if WIDTHS[piece] < W:
                spare = W - WIDTHS[piece]
                for half in range(8):
                    o[k, h, half, :, pl.ds(WIDTHS[piece], spare)] = jnp.zeros((32, spare), BF16)
            p2 = ring[k][2]
            push(0, o.at[k, h, 2 * p2], ra.at[k, 0, c], ra_sem.at[k, 0], device(order[0], 1, h))
            push(0, o.at[k, h, 2 * p2 + 1], ra.at[k, 1, c], ra_sem.at[k, 1], device(order[0], 3, h))
    for k, order in enumerate(ORDERS):
        p, p1, _, p3 = ring[k]
        push(0, o.at[k, other, 2 * p1], ra.at[k, 0, 2], ra_sem.at[k, 0], partner)
        push(0, o.at[k, other, 2 * p3 + 1], ra.at[k, 1, 2], ra_sem.at[k, 1], partner)
    for k, order in enumerate(ORDERS):
        p, p1, _, p3 = ring[k]
        for h in range(2):
            push(1, o.at[k, h, 2 * p1 + 1], rb1.at[k, c], rb1_sem.at[k], device(order[0], 1, h))
            push(1, o.at[k, h, 2 * p3], rb1.at[k, 2 + c], rb1_sem.at[k], device(order[0], 3, h))
    for k in range(3):
        push(1, o.at[k, other, pl.ds(2 * ring[k][0], 2)], rb1.at[k, pl.ds(4, 2)], rb1_sem.at[k], partner)

    def rest_column(j, carry):
        cols = lane_tile(j * LANES)
        for top in range(0, ROWS, 16):
            rows = pl.ds(top, 16)
            value, size = comb[rows, cols], scale[rows]
            wn[rows, cols] = (value - jnp.where(value >= 0, size, -size)).astype(BF16)
        return carry

    lax.fori_loop(0, COLS // LANES, rest_column, 0)

    for k, order in enumerate(ORDERS):
        p, p1, _, p3 = ring[k]
        for d in range(2):
            arrived(ra.at[k, d], ra_sem.at[k, d])
            for half in range(2):
                rows = pl.ds(16 * half, 16)
                sb2[k, d, rows] = (
                    (o[k, c, 2 * p1 if d == 0 else 2 * p3 + 1, rows].astype(F32) + ra[k, d, 2, rows].astype(F32))
                    + (ra[k, d, 0, rows].astype(F32) + ra[k, d, 1, rows].astype(F32))
                )
            push(2, sb2.at[k, d], rb2.at[k, d], rb2_sem.at[k], device(order[0], 1 if d == 0 else 3, c))

    for k, order in enumerate(ORDERS):
        p, q = ring[k][0], pos[order[1]]
        arrived(rb1.at[k], rb1_sem.at[k])
        arrived(rb2.at[k], rb2_sem.at[k])
        for d in range(2):
            for half in range(2):
                rows = pl.ds(16 * half, 16)
                s1[k, 2 * d + half] = (
                    (o[k, c, 2 * p + d, rows].astype(F32) + rb1[k, 4 + d, rows].astype(F32))
                    + (rb1[k, 2 - 2 * d, rows].astype(F32) + rb1[k, 3 - 2 * d, rows].astype(F32))
                    + rb2[k, d, rows]
                )
        for delta in (2, 1, 3):
            push(3, s1.at[k, step(q, delta)], r2.at[k, delta - 1], r2_sem.at[k], device(order[1], delta, c))

    def rate_column(j, carry):
        cols = lane_tile(j * LANES)
        for top in range(0, ROWS, 16):
            rows = pl.ds(top, 16)
            rate[rows, cols] = 0.5 / (jnp.sqrt(vv[rows, cols].astype(F32)) + 1e-08)
        return carry

    v_copy.wait()
    lax.fori_loop(0, COLS // LANES, rate_column, 0)

    for k, order in enumerate(ORDERS):
        q, r = pos[order[1]], pos[order[2]]
        arrived(r2.at[k], r2_sem.at[k])
        st[k] = (s1[k, q] + r2[k, 0]) + (r2[k, 1] + r2[k, 2])
        for i in range(8):
            s2[k, i] = st[k, pl.ds(2 * i, 2), :]
        for delta in (2, 1, 3):
            for core in range(2):
                src, dst = s2.at[k, 2 * step(r, delta) + core], r3.at[k, 2 * delta + c]
                push(4, src, dst, r3_sem.at[k], device(order[2], delta, core))
        push(4, s2.at[k, 2 * r + other], r3.at[k, c], r3_sem.at[k], partner)
        r3[k, c] = s2[k, 2 * r + c]

    se_copy.wait()
    squares = jnp.zeros((2, LANES), F32)
    for piece in range(6):
        k, h = divmod(piece, 2)
        if h == 0:
            arrived(r3.at[k, pl.ds(0, 7)], r3_sem.at[k])
        width = WIDTHS[piece]
        cols = pl.ds(0, width)
        total = (r3[k, h, :, cols] + r3[k, 2 + h, :, cols]) + (r3[k, 4 + h, :, cols] + r3[k, 6 + h, :, cols])
        served = total * (1.0 / N_DEV) + se[:, pl.ds(piece * W, width)].astype(F32)
        sv[piece, :, cols] = served
        for t in range(width // LANES):
            part = served[:, t * LANES : (t + 1) * LANES]
            squares = squares + part * part
    total = jnp.sum(jnp.sum(squares, axis=1, keepdims=True), axis=0, keepdims=True)
    size = jnp.sqrt(total * (1.0 / N_BLOCK)).astype(BF16).astype(F32)
    for piece in range(6):
        k, h = divmod(piece, 2)
        width = WIDTHS[piece]
        cols = pl.ds(0, width)
        served = sv[piece, :, cols]
        level = jnp.broadcast_to(size, (2, width))
        comp = jnp.where(served >= 0, level, -level)
        sn[:, pl.ds(piece * W, width)] = (served - comp).astype(BF16)
        mb[k, h, :, cols] = comp.astype(BF16)
        if width < W:
            mb[k, h, :, pl.ds(width, W - width)] = jnp.zeros((2, W - width), BF16)

    for k, order in enumerate(ORDERS):
        r = pos[order[2]]
        mine = 2 * r + c
        for delta in (2, 1, 3):
            for h in range(2):
                push(5, mb.at[k, h], rq.at[k, mine], rq_sem.at[k], device(order[2], delta, h))
        push(5, mb.at[k, other], rq.at[k, mine], rq_sem.at[k], partner)
        rq[k, mine] = mb[k, c]

    def spread(k, at, group):
        order = ORDERS[k]
        view = m.at[k, c, ring[k][0], at]
        for delta in (2, 1, 3):
            push(7, view, view, q3_sem.at[k, group, delta - 1], device(order[0], delta, c))
        push(8, view, view, d_sem.at[0], partner)

    for k, order in enumerate(ORDERS):
        p, q = pos[order[0]], pos[order[1]]
        arrived(rq.at[k, pl.ds(0, 7)], rq_sem.at[k])
        for i in range(8):
            st[k, pl.ds(2 * i, 2), :] = rq[k, i].astype(F32)
        m[k, c, p, q] = st[k].astype(BF16)
        view = m.at[k, c, p, q]
        for delta in (2, 1, 3):
            push(6, view, view, q2_sem.at[k, delta - 1], device(order[1], delta, c))
    for k, order in enumerate(ORDERS):
        spread(k, pos[order[1]], 0)
    for delta in (1, 3, 2):
        for k, order in enumerate(ORDERS):
            at = step(pos[order[1]], 4 - delta)
            arrived(m.at[k, c, pos[order[0]], at], q2_sem.at[k, delta - 1])
            spread(k, at, 1 if delta % 2 else 2)
    for group, tiles in enumerate(((0,), (1, 3), (2,))):
        for delta in (1, 3, 2):
            for k, order in enumerate(ORDERS):
                at, q = step(pos[order[0]], 4 - delta), pos[order[1]]
                arrived(m.at[k, c, at, pl.ds(0, len(tiles))], q3_sem.at[k, group, delta - 1])
                for shift in tiles:
                    view = m.at[k, c, at, step(q, shift)]
                    push(8, view, view, d_sem.at[0], partner)
    arrived(m.at[:, other], d_sem.at[0])
    p_copy.wait()
    for stage, alike in enumerate((
        ra, rb1, rb2, r2, r3.at[:, pl.ds(0, 7)], rq.at[:, pl.ds(0, 7)],
        m.at[:, 0, 0, pl.ds(0, 3)], m.at[:, 0, pl.ds(0, 3)], m.at[:, 0],
    )):
        left(stage, alike)


def update_kernel(m, wn, sn, rate, pv, params_next, momentum_next, worker_next, server_next, pn, mn, sem):
    whole = [
        pltpu.make_async_copy(wn, worker_next, sem.at[0]),
        pltpu.make_async_copy(sn, server_next, sem.at[1]),
    ]
    for copy in whole:
        copy.start()
    for piece in range(6):
        k, h = divmod(piece, 2)

        def column(j, carry, piece=piece, k=k, h=h):
            src, dst = lane_tile(j * LANES), lane_tile(piece * W + j * LANES)
            for outer in range(4):
                tiles = []
                for i in range(4):
                    far, near = (i, outer) if k == 2 else (outer, i)
                    tile = m[k, h, far, near, :, src].astype(F32)
                    tiles.append([tile[:8], tile[8:]])
                if k != 0:
                    tiles = swap_granules(tiles)
                for inner in range(4):
                    x, z = (inner, outer) if k == 1 else (outer, inner)
                    rows = pl.ds(16 * (4 * x + z), 16)
                    value = jnp.concatenate(tiles[inner], 0)
                    mn[rows, dst] = value.astype(BF16)
                    pn[rows, dst] = pv[rows, dst] - value * rate[rows, dst]
            return carry

        lax.fori_loop(0, WIDTHS[piece] // LANES, column, 0)
        cols = pl.ds(piece * W, WIDTHS[piece])
        pltpu.make_async_copy(pn.at[:, cols], params_next.at[:, cols], sem.at[2]).start()
        pltpu.make_async_copy(mn.at[:, cols], momentum_next.at[:, cols], sem.at[3]).start()
    whole += [
        pltpu.make_async_copy(pn, params_next, sem.at[2]),
        pltpu.make_async_copy(mn, momentum_next, sem.at[3]),
    ]
    for copy in whole:
        copy.wait()


def local(gradients, momentum, worker_error, server_error, params, variance):
    hbm = pl.BlockSpec(memory_space=pltpu.HBM)
    vmem = pl.BlockSpec(memory_space=pltpu.VMEM)
    dma = pltpu.SemaphoreType.DMA
    whole = (ROWS, COLS)
    own = (ROWS // N_DEV, COLS)
    gathered, server_next, worker_next, rate, held = pl.pallas_call(
        step_kernel,
        out_shape=(
            pltpu.VMEM((3, 2, 4, 4, 16, W), BF16),
            pltpu.VMEM(own, BF16),
            pltpu.VMEM(whole, BF16),
            pltpu.VMEM(whole, F32),
            pltpu.VMEM(whole, F32),
        ),
        in_specs=[hbm] * 6,
        out_specs=(vmem,) * 5,
        scratch_shapes=[
            pltpu.VMEM((3, ROWS, COLS), BF16),
            pltpu.VMEM(whole, BF16),
            pltpu.VMEM(own, BF16),
            pltpu.VMEM(whole, F32),
            pltpu.VMEM((ROWS, LANES), F32),
            pltpu.VMEM((3, 2, 8, 32, W), BF16),
            pltpu.VMEM((3, 2, 3, 32, W), BF16),
            pltpu.VMEM((3, 6, 32, W), BF16),
            pltpu.VMEM((3, 2, 32, W), F32),
            pltpu.VMEM((3, 2, 32, W), F32),
            pltpu.VMEM((3, 4, 16, W), F32),
            pltpu.VMEM((3, 3, 16, W), F32),
            pltpu.VMEM((3, 16, W), F32),
            pltpu.VMEM((3, 8, 2, W), F32),
            pltpu.VMEM((3, 8, 2, W), F32),
            pltpu.VMEM((6, 2, W), F32),
            pltpu.VMEM((3, 2, 2, W), BF16),
            pltpu.VMEM((3, 8, 2, W), BF16),
            dma((ROWS // CHUNK,)),
            dma((3,)),
            dma((9,)),
            dma((3, 2)),
            dma((3,)),
            dma((3,)),
            dma((3,)),
            dma((3,)),
            dma((3,)),
            dma((3, 3)),
            dma((3, 3, 3)),
            dma((1,)),
        ],
        compiler_params=pltpu.CompilerParams(
            collective_id=0, has_side_effects=True, vmem_limit_bytes=VMEM_STEP
        ),
        name="step",
    )(
        *(
            pltpu.with_memory_space_constraint(a, pltpu.HBM)
            for a in (
                gradients.reshape(whole), momentum, worker_error.reshape(whole), server_error, params, variance
            )
        )
    )

    params_next, momentum_next, worker_next, server_next = pl.pallas_call(
        update_kernel,
        out_shape=(
            jax.ShapeDtypeStruct(whole, F32),
            jax.ShapeDtypeStruct(whole, BF16),
            jax.ShapeDtypeStruct(whole, BF16),
            jax.ShapeDtypeStruct(own, BF16),
        ),
        in_specs=[vmem] * 5,
        out_specs=(hbm,) * 4,
        scratch_shapes=[pltpu.VMEM(whole, F32), pltpu.VMEM(whole, BF16), dma((4,))],
        compiler_params=pltpu.CompilerParams(vmem_limit_bytes=VMEM_UPDATE),
        name="update",
    )(
        *(
            pltpu.with_memory_space_constraint(a, pltpu.VMEM)
            for a in (gathered, worker_next, server_next, rate, held)
        )
    )
    return (params_next, momentum_next, worker_next.reshape(1, ROWS, COLS), server_next)


def solution(mesh):
    split = Mesh(mesh.devices.reshape(4, 4, 4, 2), DP)
    in_specs = (P(DP, None, None), P(), P(DP, None, None), P(DP, None), P(), P())
    out_specs = (P(), P(), P(DP, None, None), P(DP, None))
    return jax.shard_map(local, mesh=split, in_specs=in_specs, out_specs=out_specs, check_vma=False)
```

```python
import jax
import jax.numpy as jnp
from jax import lax
from jax.experimental import pallas as pl
from jax.experimental.pallas import tpu as pltpu
from jax.sharding import Mesh
from jax.sharding import PartitionSpec as P

MESH = pl.DeviceIdType.MESH
F32, BF16 = jnp.float32, jnp.bfloat16
DP = ("dp_0", "dp_1", "dp_2", "dp_3")
ORDERS = ((0, 1, 2), (1, 2, 0), (2, 0, 1))
ROWS, COLS, N_DEV = 256, 5120, 128
LANES = 128
W = 7 * LANES
WIDTHS = (W, W, W, W, W, COLS - 5 * W)
N_BLOCK = (ROWS // N_DEV) * COLS
CHUNK = 64
VMEM_STEP, VMEM_UPDATE = 26 * 2**20, 9 * 2**20


def lane_tile(start):
    return pl.ds(pl.multiple_of(start, LANES), LANES)


def swap_granules(tiles):
    low = lax.broadcasted_iota(jnp.int32, (8, LANES), 0) < 4
    swapped = []
    for i in range(4):
        pairs = []
        for first, second in ((tiles[0], tiles[1]), (tiles[2], tiles[3])):
            a, b = first[i // 2], second[i // 2]
            if i % 2 == 0:
                pairs.append(jnp.where(low, a, pltpu.roll(b, 4, 0)))
            else:
                pairs.append(jnp.where(low, pltpu.roll(a, 4, 0), b))
        swapped.append(pairs)
    return swapped


def step_kernel(
    g_hbm, m_hbm, e_hbm, se_hbm, p_hbm, v_hbm, m, sn, wn, rate, pv,
    gme, vv, se, comb, scale, o, ra, rb1, rb2, sb2, s1, r2, st, s2, r3, sv, mb, rq,
    in_sem, aux_sem, send_sem, ra_sem, rb1_sem, rb2_sem, r2_sem, r3_sem, rq_sem, q3_sem, d_sem,
):
    pos = [lax.axis_index(DP[a]) for a in range(3)]
    c = lax.axis_index(DP[3])
    other = 1 - c

    def step(v, d):
        return lax.rem(v + d, 4)

    def device(axis, delta, core):
        at = list(pos)
        if not isinstance(delta, int) or delta:
            at[axis] = step(pos[axis], delta)
        return (*at, core)

    def push(stage, src, dst, sem, to):
        pltpu.make_async_remote_copy(
            src_ref=src, dst_ref=dst, send_sem=send_sem.at[stage], recv_sem=sem,
            device_id=to, device_id_type=MESH,
        ).start()

    def left(stage, alike):
        pltpu.make_async_remote_copy(
            src_ref=alike, dst_ref=alike, send_sem=send_sem.at[stage], recv_sem=d_sem.at[0],
            device_id=device(0, 0, other), device_id_type=MESH,
        ).wait_send()

    def arrived(dst, sem):
        pltpu.make_async_remote_copy(
            src_ref=dst, dst_ref=dst, send_sem=send_sem.at[0], recv_sem=sem,
            device_id=device(0, 0, other), device_id_type=MESH,
        ).wait_recv()

    barrier = pltpu.get_barrier_semaphore()
    for i in range(ROWS // CHUNK):
        rows = pl.ds(i * CHUNK, CHUNK)
        for n, src in enumerate((g_hbm, m_hbm, e_hbm)):
            pltpu.make_async_copy(src.at[rows], gme.at[n, rows], in_sem.at[i]).start()

    peers = [(*pos, other)]
    for x in range(4):
        for z in range(4):
            for y in range(4):
                if x * z * y == 0 and x + z + y > 0:
                    chip = (step(pos[0], x), step(pos[1], z), step(pos[2], y))
                    peers += [(*chip, 0), (*chip, 1)]
    for peer in peers:
        pl.semaphore_signal(barrier, inc=1, device_id=peer, device_id_type=MESH)

    even = lax.broadcasted_iota(jnp.int32, (8, LANES), 0) % 2 == 0
    for i in range(ROWS // CHUNK):
        rows = pl.ds(i * CHUNK, CHUNK)
        pltpu.make_async_copy(gme.at[:, rows], gme.at[:, rows], in_sem.at[i]).wait()

        def square(t, acc, rows=rows):
            cols = lane_tile(t * LANES)
            value = (
                0.875 * gme[1, rows, cols].astype(F32)
                + 0.125 * gme[0, rows, cols].astype(F32)
                + gme[2, rows, cols].astype(F32)
            )
            comb[rows, cols] = value
            return acc + value * value

        acc = lax.fori_loop(0, COLS // LANES, square, jnp.zeros((CHUNK, LANES), F32), unroll=8)
        for s in range(CHUNK // 8):
            row = jnp.sum(acc[8 * s : 8 * s + 8], axis=1, keepdims=True)
            row = jnp.broadcast_to(row, (8, LANES))
            both = row + jnp.where(even, pltpu.roll(row, 7, 0), pltpu.roll(row, 1, 0))
            rounded = jnp.sqrt(both * (1.0 / N_BLOCK)).astype(BF16)
            scale[pl.ds(i * CHUNK + 8 * s, 8)] = rounded.astype(F32)

    se_copy = pltpu.make_async_copy(se_hbm, se, aux_sem.at[0])
    v_copy = pltpu.make_async_copy(v_hbm, vv, aux_sem.at[1])
    p_copy = pltpu.make_async_copy(p_hbm, pv, aux_sem.at[2])
    for copy in (se_copy, v_copy, p_copy):
        copy.start()
    pl.semaphore_wait(barrier, len(peers))

    partner = device(0, 0, other)
    ring = [tuple(step(pos[order[0]], d) for d in range(4)) for order in ORDERS]

    for h in range(2):
        for k, order in enumerate(ORDERS):
            piece = 2 * k + h

            def column(j, carry, piece=piece, k=k, h=h):
                src, dst = lane_tile(piece * W + j * LANES), lane_tile(j * LANES)
                for outer in range(4):
                    tiles = []
                    for inner in range(4):
                        x, z = (inner, outer) if k == 1 else (outer, inner)
                        parts = []
                        for s in range(2):
                            rows = pl.ds(16 * (4 * x + z) + 8 * s, 8)
                            size = scale[rows]
                            parts.append(jnp.where(comb[rows, src] >= 0, size, -size))
                        tiles.append(parts)
                    if k != 0:
                        tiles = swap_granules(tiles)
                    for i in range(4):
                        far, near = (i, outer) if k == 2 else (outer, i)
                        half, row = 2 * far + near // 2, (near % 2) * 16
                        o[k, h, half, pl.ds(row, 16), dst] = jnp.concatenate(tiles[i], 0).astype(BF16)
                return carry

            lax.fori_loop(0, WIDTHS[piece] // LANES, column, 0)
            if WIDTHS[piece] < W:
                spare = W - WIDTHS[piece]
                for half in range(8):
                    o[k, h, half, :, pl.ds(WIDTHS[piece], spare)] = jnp.zeros((32, spare), BF16)
            p2 = ring[k][2]
            push(0, o.at[k, h, 2 * p2], ra.at[k, 0, c], ra_sem.at[k, 0], device(order[0], 1, h))
            push(0, o.at[k, h, 2 * p2 + 1], ra.at[k, 1, c], ra_sem.at[k, 1], device(order[0], 3, h))
    for k, order in enumerate(ORDERS):
        p, p1, _, p3 = ring[k]
        push(0, o.at[k, other, 2 * p1], ra.at[k, 0, 2], ra_sem.at[k, 0], partner)
        push(0, o.at[k, other, 2 * p3 + 1], ra.at[k, 1, 2], ra_sem.at[k, 1], partner)
    for k, order in enumerate(ORDERS):
        p, p1, _, p3 = ring[k]
        for h in range(2):
            push(1, o.at[k, h, 2 * p1 + 1], rb1.at[k, c], rb1_sem.at[k], device(order[0], 1, h))
            push(1, o.at[k, h, 2 * p3], rb1.at[k, 2 + c], rb1_sem.at[k], device(order[0], 3, h))
    for k in range(3):
        push(1, o.at[k, other, pl.ds(2 * ring[k][0], 2)], rb1.at[k, pl.ds(4, 2)], rb1_sem.at[k], partner)

    def rest_column(j, carry):
        cols = lane_tile(j * LANES)
        for top in range(0, ROWS, 16):
            rows = pl.ds(top, 16)
            value, size = comb[rows, cols], scale[rows]
            wn[rows, cols] = (value - jnp.where(value >= 0, size, -size)).astype(BF16)
        return carry

    lax.fori_loop(0, COLS // LANES, rest_column, 0)

    for half in range(2):
        rows = pl.ds(16 * half, 16)
        for k, order in enumerate(ORDERS):
            p, p1, _, p3 = ring[k]
            for d in range(2):
                if half == 0:
                    arrived(ra.at[k, d], ra_sem.at[k, d])
                sb2[k, d, rows] = (
                    (o[k, c, 2 * p1 if d == 0 else 2 * p3 + 1, rows].astype(F32) + ra[k, d, 2, rows].astype(F32))
                    + (ra[k, d, 0, rows].astype(F32) + ra[k, d, 1, rows].astype(F32))
                )
                to = device(order[0], 1 if d == 0 else 3, c)
                push(2, sb2.at[k, d, rows], rb2.at[k, d, rows], rb2_sem.at[k, half], to)

    for half in range(2):
        rows = pl.ds(16 * half, 16)
        for k, order in enumerate(ORDERS):
            p, q = ring[k][0], pos[order[1]]
            if half == 0:
                arrived(rb1.at[k], rb1_sem.at[k])
            arrived(rb2.at[k, 0], rb2_sem.at[k, half])
            for d in range(2):
                s1[k, 2 * d + half] = (
                    (o[k, c, 2 * p + d, rows].astype(F32) + rb1[k, 4 + d, rows].astype(F32))
                    + (rb1[k, 2 - 2 * d, rows].astype(F32) + rb1[k, 3 - 2 * d, rows].astype(F32))
                    + rb2[k, d, rows]
                )
            for to in (half, 2 + half):

                @pl.when(q != to)
                def _(k=k, order=order, q=q, to=to):
                    delta = step(to + 4, -q)
                    push(3, s1.at[k, to], r2.at[k, delta - 1], r2_sem.at[k], device(order[1], delta, c))

    def rate_column(j, carry):
        cols = lane_tile(j * LANES)
        for top in range(0, ROWS, 16):
            rows = pl.ds(top, 16)
            rate[rows, cols] = 0.5 / (jnp.sqrt(vv[rows, cols].astype(F32)) + 1e-08)
        return carry

    v_copy.wait()
    lax.fori_loop(0, COLS // LANES, rate_column, 0)

    for k, order in enumerate(ORDERS):
        q, r = pos[order[1]], pos[order[2]]
        arrived(r2.at[k], r2_sem.at[k])
        st[k] = (s1[k, q] + r2[k, 0]) + (r2[k, 1] + r2[k, 2])
        for i in range(8):
            s2[k, i] = st[k, pl.ds(2 * i, 2), :]
        for delta in (2, 1, 3):
            for core in range(2):
                src, dst = s2.at[k, 2 * step(r, delta) + core], r3.at[k, 2 * delta + c]
                push(4, src, dst, r3_sem.at[k], device(order[2], delta, core))
        push(4, s2.at[k, 2 * r + other], r3.at[k, c], r3_sem.at[k], partner)
        r3[k, c] = s2[k, 2 * r + c]

    se_copy.wait()
    squares = jnp.zeros((2, LANES), F32)
    for piece in range(6):
        k, h = divmod(piece, 2)
        if h == 0:
            arrived(r3.at[k, pl.ds(0, 7)], r3_sem.at[k])
        width = WIDTHS[piece]
        cols = pl.ds(0, width)
        total = (r3[k, h, :, cols] + r3[k, 2 + h, :, cols]) + (r3[k, 4 + h, :, cols] + r3[k, 6 + h, :, cols])
        served = total * (1.0 / N_DEV) + se[:, pl.ds(piece * W, width)].astype(F32)
        sv[piece, :, cols] = served
        for t in range(width // LANES):
            part = served[:, t * LANES : (t + 1) * LANES]
            squares = squares + part * part
    total = jnp.sum(jnp.sum(squares, axis=1, keepdims=True), axis=0, keepdims=True)
    size = jnp.sqrt(total * (1.0 / N_BLOCK)).astype(BF16).astype(F32)
    for piece in range(6):
        k, h = divmod(piece, 2)
        width = WIDTHS[piece]
        cols = pl.ds(0, width)
        served = sv[piece, :, cols]
        level = jnp.broadcast_to(size, (2, width))
        comp = jnp.where(served >= 0, level, -level)
        sn[:, pl.ds(piece * W, width)] = (served - comp).astype(BF16)
        mb[k, h, :, cols] = comp.astype(BF16)
        if width < W:
            mb[k, h, :, pl.ds(width, W - width)] = jnp.zeros((2, W - width), BF16)

    def place(k, q_shift, r_shift, core):
        at = list(pos)
        at[ORDERS[k][1]] = step(at[ORDERS[k][1]], q_shift)
        at[ORDERS[k][2]] = step(at[ORDERS[k][2]], r_shift)
        return (*at, core)

    for q_shift in (0, 1, 3, 2):
        for r_shift in (2, 1, 3, 0):
            for k, order in enumerate(ORDERS):
                q, mine = pos[order[1]], 2 * pos[order[2]] + c
                sem = rq_sem.at[k, (0, 1, 2, 1)[q_shift]]
                if q_shift or r_shift:
                    for h in range(2):
                        push(8 if q_shift else 5, mb.at[k, h], rq.at[k, q, mine], sem, place(k, q_shift, r_shift, h))
                else:
                    push(5, mb.at[k, other], rq.at[k, q, mine], sem, partner)
                    rq[k, q, mine] = mb[k, c]

    def spread(k, at, group):
        order = ORDERS[k]
        view = m.at[k, c, ring[k][0], at]
        for delta in (2, 1, 3):
            push(6, view, view, q3_sem.at[k, group], device(order[0], delta, c))
        push(7, view, view, d_sem.at[0], partner)

    for group, shifts in enumerate(((0,), (1, 3), (2,))):
        for k, order in enumerate(ORDERS):
            q = pos[order[1]]
            arrived(rq.at[k, 0, pl.ds(0, 7)] if group == 0 else rq.at[k, pl.ds(0, len(shifts))], rq_sem.at[k, group])
            for shift in shifts:
                at = step(q, shift)
                for i in range(8):
                    st[k, pl.ds(2 * i, 2), :] = rq[k, at, i].astype(F32)
                m[k, c, pos[order[0]], at] = st[k].astype(BF16)
            for shift in shifts:
                spread(k, step(q, shift), group)
    for group, tiles in enumerate(((0,), (1, 3), (2,))):
        for k, order in enumerate(ORDERS):
            arrived(m.at[k, 0, pl.ds(0, 3), pl.ds(0, len(tiles))], q3_sem.at[k, group])
            for delta in (1, 3, 2):
                at, q = step(pos[order[0]], 4 - delta), pos[order[1]]
                for shift in tiles:
                    view = m.at[k, c, at, step(q, shift)]
                    push(7, view, view, d_sem.at[0], partner)
    arrived(m.at[:, other], d_sem.at[0])
    p_copy.wait()
    for stage, alike in enumerate((
        ra, rb1, rb2, r2, r3.at[:, pl.ds(0, 7)], rq.at[:, 0, pl.ds(0, 7)],
        m.at[:, 0, pl.ds(0, 3)], m.at[:, 0], rq.at[:, pl.ds(0, 3)],
    )):
        left(stage, alike)


def update_kernel(m, wn, sn, rate, pv, params_next, momentum_next, worker_next, server_next, pn, mn, sem):
    whole = [
        pltpu.make_async_copy(wn, worker_next, sem.at[0]),
        pltpu.make_async_copy(sn, server_next, sem.at[1]),
    ]
    for copy in whole:
        copy.start()
    for piece in range(6):
        k, h = divmod(piece, 2)

        def column(j, carry, piece=piece, k=k, h=h):
            src, dst = lane_tile(j * LANES), lane_tile(piece * W + j * LANES)
            for outer in range(4):
                tiles = []
                for i in range(4):
                    far, near = (i, outer) if k == 2 else (outer, i)
                    tile = m[k, h, far, near, :, src].astype(F32)
                    tiles.append([tile[:8], tile[8:]])
                if k != 0:
                    tiles = swap_granules(tiles)
                for inner in range(4):
                    x, z = (inner, outer) if k == 1 else (outer, inner)
                    rows = pl.ds(16 * (4 * x + z), 16)
                    value = jnp.concatenate(tiles[inner], 0)
                    mn[rows, dst] = value.astype(BF16)
                    pn[rows, dst] = pv[rows, dst] - value * rate[rows, dst]
            return carry

        lax.fori_loop(0, WIDTHS[piece] // LANES, column, 0)
        cols = pl.ds(piece * W, WIDTHS[piece])
        pltpu.make_async_copy(pn.at[:, cols], params_next.at[:, cols], sem.at[2]).start()
        pltpu.make_async_copy(mn.at[:, cols], momentum_next.at[:, cols], sem.at[3]).start()
    whole += [
        pltpu.make_async_copy(pn, params_next, sem.at[2]),
        pltpu.make_async_copy(mn, momentum_next, sem.at[3]),
    ]
    for copy in whole:
        copy.wait()


def local(gradients, momentum, worker_error, server_error, params, variance):
    hbm = pl.BlockSpec(memory_space=pltpu.HBM)
    vmem = pl.BlockSpec(memory_space=pltpu.VMEM)
    dma = pltpu.SemaphoreType.DMA
    whole = (ROWS, COLS)
    own = (ROWS // N_DEV, COLS)
    gathered, server_next, worker_next, rate, held = pl.pallas_call(
        step_kernel,
        out_shape=(
            pltpu.VMEM((3, 2, 4, 4, 16, W), BF16),
            pltpu.VMEM(own, BF16),
            pltpu.VMEM(whole, BF16),
            pltpu.VMEM(whole, F32),
            pltpu.VMEM(whole, F32),
        ),
        in_specs=[hbm] * 6,
        out_specs=(vmem,) * 5,
        scratch_shapes=[
            pltpu.VMEM((3, ROWS, COLS), BF16),
            pltpu.VMEM(whole, BF16),
            pltpu.VMEM(own, BF16),
            pltpu.VMEM(whole, F32),
            pltpu.VMEM((ROWS, LANES), F32),
            pltpu.VMEM((3, 2, 8, 32, W), BF16),
            pltpu.VMEM((3, 2, 3, 32, W), BF16),
            pltpu.VMEM((3, 6, 32, W), BF16),
            pltpu.VMEM((3, 2, 32, W), F32),
            pltpu.VMEM((3, 2, 32, W), F32),
            pltpu.VMEM((3, 4, 16, W), F32),
            pltpu.VMEM((3, 3, 16, W), F32),
            pltpu.VMEM((3, 16, W), F32),
            pltpu.VMEM((3, 8, 2, W), F32),
            pltpu.VMEM((3, 8, 2, W), F32),
            pltpu.VMEM((6, 2, W), F32),
            pltpu.VMEM((3, 2, 2, W), BF16),
            pltpu.VMEM((3, 4, 8, 2, W), BF16),
            dma((ROWS // CHUNK,)),
            dma((3,)),
            dma((9,)),
            dma((3, 2)),
            dma((3,)),
            dma((3, 2)),
            dma((3,)),
            dma((3,)),
            dma((3, 3)),
            dma((3, 3)),
            dma((1,)),
        ],
        compiler_params=pltpu.CompilerParams(
            collective_id=0, has_side_effects=True, vmem_limit_bytes=VMEM_STEP
        ),
        name="step",
    )(
        *(
            pltpu.with_memory_space_constraint(a, pltpu.HBM)
            for a in (
                gradients.reshape(whole), momentum, worker_error.reshape(whole), server_error, params, variance
            )
        )
    )

    params_next, momentum_next, worker_next, server_next = pl.pallas_call(
        update_kernel,
        out_shape=(
            jax.ShapeDtypeStruct(whole, F32),
            jax.ShapeDtypeStruct(whole, BF16),
            jax.ShapeDtypeStruct(whole, BF16),
            jax.ShapeDtypeStruct(own, BF16),
        ),
        in_specs=[vmem] * 5,
        out_specs=(hbm,) * 4,
        scratch_shapes=[pltpu.VMEM(whole, F32), pltpu.VMEM(whole, BF16), dma((4,))],
        compiler_params=pltpu.CompilerParams(vmem_limit_bytes=VMEM_UPDATE),
        name="update",
    )(
        *(
            pltpu.with_memory_space_constraint(a, pltpu.VMEM)
            for a in (gathered, worker_next, server_next, rate, held)
        )
    )
    return (params_next, momentum_next, worker_next.reshape(1, ROWS, COLS), server_next)


def solution(mesh):
    split = Mesh(mesh.devices.reshape(4, 4, 4, 2), DP)
    in_specs = (P(DP, None, None), P(), P(DP, None, None), P(DP, None), P(), P())
    out_specs = (P(), P(), P(DP, None, None), P(DP, None))
    return jax.shard_map(local, mesh=split, in_specs=in_specs, out_specs=out_specs, check_vma=False)
```

```python
import jax
import jax.numpy as jnp
from jax import lax
from jax.experimental import pallas as pl
from jax.experimental.pallas import tpu as pltpu
from jax.sharding import Mesh
from jax.sharding import PartitionSpec as P

MESH = pl.DeviceIdType.MESH
F32, BF16 = jnp.float32, jnp.bfloat16
DP = ("dp_0", "dp_1", "dp_2", "dp_3")
ORDERS = ((0, 1, 2), (1, 2, 0), (2, 0, 1))
ROWS, COLS, N_DEV = 256, 5120, 128
LANES = 128
W = 7 * LANES
WIDTHS = (W, W, W, W, W, COLS - 5 * W)
N_BLOCK = (ROWS // N_DEV) * COLS
CHUNK = 64
VMEM_STEP, VMEM_UPDATE = 26 * 2**20, 9 * 2**20


def lane_tile(start):
    return pl.ds(pl.multiple_of(start, LANES), LANES)


def swap_granules(tiles):
    low = lax.broadcasted_iota(jnp.int32, (8, LANES), 0) < 4
    swapped = []
    for i in range(4):
        pairs = []
        for first, second in ((tiles[0], tiles[1]), (tiles[2], tiles[3])):
            a, b = first[i // 2], second[i // 2]
            if i % 2 == 0:
                pairs.append(jnp.where(low, a, pltpu.roll(b, 4, 0)))
            else:
                pairs.append(jnp.where(low, pltpu.roll(a, 4, 0), b))
        swapped.append(pairs)
    return swapped


def step_kernel(
    g_hbm, m_hbm, e_hbm, se_hbm, p_hbm, v_hbm, m, sn, wn, rate, pv,
    gme, vv, se, comb, scale, o, ra, rb1, rb2, sb2, s1, r2, st, s2, r3, sv, mb, rq,
    in_sem, aux_sem, send_sem, ra_sem, rb1_sem, rb2_sem, r2_sem, r3_sem, rq_sem, q3_sem, d_sem,
):
    pos = [lax.axis_index(DP[a]) for a in range(3)]
    c = lax.axis_index(DP[3])
    other = 1 - c

    def step(v, d):
        return lax.rem(v + d, 4)

    def device(axis, delta, core):
        at = list(pos)
        if not isinstance(delta, int) or delta:
            at[axis] = step(pos[axis], delta)
        return (*at, core)

    def push(stage, src, dst, sem, to):
        pltpu.make_async_remote_copy(
            src_ref=src, dst_ref=dst, send_sem=send_sem.at[stage], recv_sem=sem,
            device_id=to, device_id_type=MESH,
        ).start()

    def left(stage, alike):
        pltpu.make_async_remote_copy(
            src_ref=alike, dst_ref=alike, send_sem=send_sem.at[stage], recv_sem=d_sem.at[0],
            device_id=device(0, 0, other), device_id_type=MESH,
        ).wait_send()

    def arrived(dst, sem):
        pltpu.make_async_remote_copy(
            src_ref=dst, dst_ref=dst, send_sem=send_sem.at[0], recv_sem=sem,
            device_id=device(0, 0, other), device_id_type=MESH,
        ).wait_recv()

    barrier = pltpu.get_barrier_semaphore()
    for i in range(ROWS // CHUNK):
        rows = pl.ds(i * CHUNK, CHUNK)
        for n, src in enumerate((g_hbm, m_hbm, e_hbm)):
            pltpu.make_async_copy(src.at[rows], gme.at[n, rows], in_sem.at[i]).start()

    peers = [(*pos, other)]
    for x in range(4):
        for z in range(4):
            for y in range(4):
                if x * z * y == 0 and x + z + y > 0:
                    chip = (step(pos[0], x), step(pos[1], z), step(pos[2], y))
                    peers += [(*chip, 0), (*chip, 1)]
    for peer in peers:
        pl.semaphore_signal(barrier, inc=1, device_id=peer, device_id_type=MESH)

    even = lax.broadcasted_iota(jnp.int32, (8, LANES), 0) % 2 == 0
    for i in range(ROWS // CHUNK):
        rows = pl.ds(i * CHUNK, CHUNK)
        pltpu.make_async_copy(gme.at[:, rows], gme.at[:, rows], in_sem.at[i]).wait()

        def square(t, acc, rows=rows):
            cols = lane_tile(t * LANES)
            value = (
                0.875 * gme[1, rows, cols].astype(F32)
                + 0.125 * gme[0, rows, cols].astype(F32)
                + gme[2, rows, cols].astype(F32)
            )
            comb[rows, cols] = value
            return acc + value * value

        acc = lax.fori_loop(0, COLS // LANES, square, jnp.zeros((CHUNK, LANES), F32), unroll=8)
        for s in range(CHUNK // 8):
            row = jnp.sum(acc[8 * s : 8 * s + 8], axis=1, keepdims=True)
            row = jnp.broadcast_to(row, (8, LANES))
            both = row + jnp.where(even, pltpu.roll(row, 7, 0), pltpu.roll(row, 1, 0))
            rounded = jnp.sqrt(both * (1.0 / N_BLOCK)).astype(BF16)
            scale[pl.ds(i * CHUNK + 8 * s, 8)] = rounded.astype(F32)

    se_copy = pltpu.make_async_copy(se_hbm, se, aux_sem.at[0])
    v_copy = pltpu.make_async_copy(v_hbm, vv, aux_sem.at[1])
    p_copy = pltpu.make_async_copy(p_hbm, pv, aux_sem.at[2])
    for copy in (se_copy, v_copy, p_copy):
        copy.start()
    pl.semaphore_wait(barrier, len(peers))

    partner = device(0, 0, other)
    ring = [tuple(step(pos[order[0]], d) for d in range(4)) for order in ORDERS]

    for h in range(2):
        for k, order in enumerate(ORDERS):
            piece = 2 * k + h

            def column(j, carry, piece=piece, k=k, h=h):
                src, dst = lane_tile(piece * W + j * LANES), lane_tile(j * LANES)
                for outer in range(4):
                    tiles = []
                    for inner in range(4):
                        x, z = (inner, outer) if k == 1 else (outer, inner)
                        parts = []
                        for s in range(2):
                            rows = pl.ds(16 * (4 * x + z) + 8 * s, 8)
                            size = scale[rows]
                            parts.append(jnp.where(comb[rows, src] >= 0, size, -size))
                        tiles.append(parts)
                    if k != 0:
                        tiles = swap_granules(tiles)
                    for i in range(4):
                        far, near = (i, outer) if k == 2 else (outer, i)
                        half, row = 2 * far + near // 2, (near % 2) * 16
                        o[k, h, half, pl.ds(row, 16), dst] = jnp.concatenate(tiles[i], 0).astype(BF16)
                return carry

            lax.fori_loop(0, WIDTHS[piece] // LANES, column, 0)
            if WIDTHS[piece] < W:
                spare = W - WIDTHS[piece]
                for half in range(8):
                    o[k, h, half, :, pl.ds(WIDTHS[piece], spare)] = jnp.zeros((32, spare), BF16)
            p2 = ring[k][2]
            push(0, o.at[k, h, 2 * p2], ra.at[k, 0, c], ra_sem.at[k, 0], device(order[0], 1, h))
            push(0, o.at[k, h, 2 * p2 + 1], ra.at[k, 1, c], ra_sem.at[k, 1], device(order[0], 3, h))
    for k, order in enumerate(ORDERS):
        p, p1, _, p3 = ring[k]
        push(0, o.at[k, other, 2 * p1], ra.at[k, 0, 2], ra_sem.at[k, 0], partner)
        push(0, o.at[k, other, 2 * p3 + 1], ra.at[k, 1, 2], ra_sem.at[k, 1], partner)
    for k, order in enumerate(ORDERS):
        p, p1, _, p3 = ring[k]
        for h in range(2):
            push(1, o.at[k, h, 2 * p1 + 1], rb1.at[k, c], rb1_sem.at[k], device(order[0], 1, h))
            push(1, o.at[k, h, 2 * p3], rb1.at[k, 2 + c], rb1_sem.at[k], device(order[0], 3, h))
    for k in range(3):
        push(1, o.at[k, other, pl.ds(2 * ring[k][0], 2)], rb1.at[k, pl.ds(4, 2)], rb1_sem.at[k], partner)

    def rest_column(j, carry):
        cols = lane_tile(j * LANES)
        for top in range(0, ROWS, 16):
            rows = pl.ds(top, 16)
            value, size = comb[rows, cols], scale[rows]
            wn[rows, cols] = (value - jnp.where(value >= 0, size, -size)).astype(BF16)
        return carry

    lax.fori_loop(0, COLS // LANES, rest_column, 0)

    for half in range(2):
        rows = pl.ds(16 * half, 16)
        for k, order in enumerate(ORDERS):
            p, p1, _, p3 = ring[k]
            for d in range(2):
                if half == 0:
                    arrived(ra.at[k, d], ra_sem.at[k, d])
                sb2[k, d, rows] = (
                    (o[k, c, 2 * p1 if d == 0 else 2 * p3 + 1, rows].astype(F32) + ra[k, d, 2, rows].astype(F32))
                    + (ra[k, d, 0, rows].astype(F32) + ra[k, d, 1, rows].astype(F32))
                )
                to = device(order[0], 1 if d == 0 else 3, c)
                push(2, sb2.at[k, d, rows], rb2.at[k, d, rows], rb2_sem.at[k, half], to)

    for half in range(2):
        rows = pl.ds(16 * half, 16)
        for k, order in enumerate(ORDERS):
            p, q = ring[k][0], pos[order[1]]
            if half == 0:
                arrived(rb1.at[k], rb1_sem.at[k])
            arrived(rb2.at[k, 0], rb2_sem.at[k, half])
            for d in range(2):
                s1[k, 2 * d + half] = (
                    (o[k, c, 2 * p + d, rows].astype(F32) + rb1[k, 4 + d, rows].astype(F32))
                    + (rb1[k, 2 - 2 * d, rows].astype(F32) + rb1[k, 3 - 2 * d, rows].astype(F32))
                    + rb2[k, d, rows]
                )
            for to in (half, 2 + half):

                @pl.when(q != to)
                def _(k=k, order=order, q=q, to=to):
                    delta = step(to + 4, -q)
                    push(3, s1.at[k, to], r2.at[k, delta - 1], r2_sem.at[k], device(order[1], delta, c))

    def rate_column(j, carry):
        cols = lane_tile(j * LANES)
        for top in range(0, ROWS, 16):
            rows = pl.ds(top, 16)
            rate[rows, cols] = 0.5 / (jnp.sqrt(vv[rows, cols].astype(F32)) + 1e-08)
        return carry

    v_copy.wait()
    lax.fori_loop(0, COLS // LANES, rate_column, 0)

    for k, order in enumerate(ORDERS):
        q, r = pos[order[1]], pos[order[2]]
        arrived(r2.at[k], r2_sem.at[k])
        st[k] = (s1[k, q] + r2[k, 0]) + (r2[k, 1] + r2[k, 2])
        for i in range(8):
            s2[k, i] = st[k, pl.ds(2 * i, 2), :]
        for delta in (2, 1, 3):
            for core in range(2):
                src, dst = s2.at[k, 2 * step(r, delta) + core], r3.at[k, 2 * delta + c]
                push(4, src, dst, r3_sem.at[k], device(order[2], delta, core))
        push(4, s2.at[k, 2 * r + other], r3.at[k, c], r3_sem.at[k], partner)
        r3[k, c] = s2[k, 2 * r + c]

    se_copy.wait()
    squares = jnp.zeros((2, LANES), F32)
    for piece in range(6):
        k, h = divmod(piece, 2)
        if h == 0:
            arrived(r3.at[k, pl.ds(0, 7)], r3_sem.at[k])
        width = WIDTHS[piece]
        cols = pl.ds(0, width)
        total = (r3[k, h, :, cols] + r3[k, 2 + h, :, cols]) + (r3[k, 4 + h, :, cols] + r3[k, 6 + h, :, cols])
        served = total * (1.0 / N_DEV) + se[:, pl.ds(piece * W, width)].astype(F32)
        sv[piece, :, cols] = served
        for t in range(width // LANES):
            part = served[:, t * LANES : (t + 1) * LANES]
            squares = squares + part * part
    total = jnp.sum(jnp.sum(squares, axis=1, keepdims=True), axis=0, keepdims=True)
    size = jnp.sqrt(total * (1.0 / N_BLOCK)).astype(BF16).astype(F32)
    for piece in range(6):
        k, h = divmod(piece, 2)
        width = WIDTHS[piece]
        cols = pl.ds(0, width)
        served = sv[piece, :, cols]
        level = jnp.broadcast_to(size, (2, width))
        comp = jnp.where(served >= 0, level, -level)
        sn[:, pl.ds(piece * W, width)] = (served - comp).astype(BF16)
        mb[k, h, :, cols] = comp.astype(BF16)
        if width < W:
            mb[k, h, :, pl.ds(width, W - width)] = jnp.zeros((2, W - width), BF16)

    def place(k, q_shift, r_shift, core):
        at = list(pos)
        at[ORDERS[k][1]] = step(at[ORDERS[k][1]], q_shift)
        at[ORDERS[k][2]] = step(at[ORDERS[k][2]], r_shift)
        return (*at, core)

    for q_shift in (0, 1, 3, 2):
        for r_shift in (2, 1, 3, 0):
            for k, order in enumerate(ORDERS):
                q, mine = pos[order[1]], 2 * pos[order[2]] + c
                sem = rq_sem.at[k, (0, 1, 2, 1)[q_shift]]
                if q_shift or r_shift:
                    for h in range(2):
                        push(8 if q_shift else 5, mb.at[k, h], rq.at[k, q, mine], sem, place(k, q_shift, r_shift, h))
                else:
                    push(5, mb.at[k, other], rq.at[k, q, mine], sem, partner)
                    rq[k, q, mine] = mb[k, c]

    def spread(k, at, group):
        order = ORDERS[k]
        view = m.at[k, c, ring[k][0], at]
        for delta in (2, 1, 3):
            sem = q3_sem.at[k, 3 if group == 2 and delta == 2 else group]
            push(6, view, view, sem, device(order[0], delta, c))
        push(7, view, view, d_sem.at[0], partner)

    for group, shifts in enumerate(((0,), (1, 3), (2,))):
        for k, order in enumerate(ORDERS):
            q = pos[order[1]]
            arrived(rq.at[k, 0, pl.ds(0, 7)] if group == 0 else rq.at[k, pl.ds(0, len(shifts))], rq_sem.at[k, group])
            for shift in shifts:
                at = step(q, shift)
                for i in range(8):
                    st[k, pl.ds(2 * i, 2), :] = rq[k, at, i].astype(F32)
                m[k, c, pos[order[0]], at] = st[k].astype(BF16)
            for shift in shifts:
                spread(k, step(q, shift), group)
    for group, (tiles, deltas) in enumerate((((0,), (1, 3, 2)), ((1, 3), (1, 3, 2)), ((2,), (1, 3)), ((2,), (2,)))):
        for k, order in enumerate(ORDERS):
            arrived(m.at[k, 0, pl.ds(0, len(deltas)), pl.ds(0, len(tiles))], q3_sem.at[k, group])
            for delta in deltas:
                at, q = step(pos[order[0]], 4 - delta), pos[order[1]]
                for shift in tiles:
                    view = m.at[k, c, at, step(q, shift)]
                    push(7, view, view, d_sem.at[0], partner)
    arrived(m.at[:, other], d_sem.at[0])
    p_copy.wait()
    for stage, alike in enumerate((
        ra, rb1, rb2, r2, r3.at[:, pl.ds(0, 7)], rq.at[:, 0, pl.ds(0, 7)],
        m.at[:, 0, pl.ds(0, 3)], m.at[:, 0], rq.at[:, pl.ds(0, 3)],
    )):
        left(stage, alike)


def update_kernel(m, wn, sn, rate, pv, params_next, momentum_next, worker_next, server_next, pn, mn, sem):
    whole = [
        pltpu.make_async_copy(wn, worker_next, sem.at[0]),
        pltpu.make_async_copy(sn, server_next, sem.at[1]),
    ]
    for copy in whole:
        copy.start()
    for piece in range(6):
        k, h = divmod(piece, 2)

        def column(j, carry, piece=piece, k=k, h=h):
            src, dst = lane_tile(j * LANES), lane_tile(piece * W + j * LANES)
            for outer in range(4):
                tiles = []
                for i in range(4):
                    far, near = (i, outer) if k == 2 else (outer, i)
                    tile = m[k, h, far, near, :, src].astype(F32)
                    tiles.append([tile[:8], tile[8:]])
                if k != 0:
                    tiles = swap_granules(tiles)
                for inner in range(4):
                    x, z = (inner, outer) if k == 1 else (outer, inner)
                    rows = pl.ds(16 * (4 * x + z), 16)
                    value = jnp.concatenate(tiles[inner], 0)
                    mn[rows, dst] = value.astype(BF16)
                    pn[rows, dst] = pv[rows, dst] - value * rate[rows, dst]
            return carry

        lax.fori_loop(0, WIDTHS[piece] // LANES, column, 0)
        cols = pl.ds(piece * W, WIDTHS[piece])
        pltpu.make_async_copy(pn.at[:, cols], params_next.at[:, cols], sem.at[2]).start()
        pltpu.make_async_copy(mn.at[:, cols], momentum_next.at[:, cols], sem.at[3]).start()
    whole += [
        pltpu.make_async_copy(pn, params_next, sem.at[2]),
        pltpu.make_async_copy(mn, momentum_next, sem.at[3]),
    ]
    for copy in whole:
        copy.wait()


def local(gradients, momentum, worker_error, server_error, params, variance):
    hbm = pl.BlockSpec(memory_space=pltpu.HBM)
    vmem = pl.BlockSpec(memory_space=pltpu.VMEM)
    dma = pltpu.SemaphoreType.DMA
    whole = (ROWS, COLS)
    own = (ROWS // N_DEV, COLS)
    gathered, server_next, worker_next, rate, held = pl.pallas_call(
        step_kernel,
        out_shape=(
            pltpu.VMEM((3, 2, 4, 4, 16, W), BF16),
            pltpu.VMEM(own, BF16),
            pltpu.VMEM(whole, BF16),
            pltpu.VMEM(whole, F32),
            pltpu.VMEM(whole, F32),
        ),
        in_specs=[hbm] * 6,
        out_specs=(vmem,) * 5,
        scratch_shapes=[
            pltpu.VMEM((3, ROWS, COLS), BF16),
            pltpu.VMEM(whole, BF16),
            pltpu.VMEM(own, BF16),
            pltpu.VMEM(whole, F32),
            pltpu.VMEM((ROWS, LANES), F32),
            pltpu.VMEM((3, 2, 8, 32, W), BF16),
            pltpu.VMEM((3, 2, 3, 32, W), BF16),
            pltpu.VMEM((3, 6, 32, W), BF16),
            pltpu.VMEM((3, 2, 32, W), F32),
            pltpu.VMEM((3, 2, 32, W), F32),
            pltpu.VMEM((3, 4, 16, W), F32),
            pltpu.VMEM((3, 3, 16, W), F32),
            pltpu.VMEM((3, 16, W), F32),
            pltpu.VMEM((3, 8, 2, W), F32),
            pltpu.VMEM((3, 8, 2, W), F32),
            pltpu.VMEM((6, 2, W), F32),
            pltpu.VMEM((3, 2, 2, W), BF16),
            pltpu.VMEM((3, 4, 8, 2, W), BF16),
            dma((ROWS // CHUNK,)),
            dma((3,)),
            dma((9,)),
            dma((3, 2)),
            dma((3,)),
            dma((3, 2)),
            dma((3,)),
            dma((3,)),
            dma((3, 3)),
            dma((3, 4)),
            dma((1,)),
        ],
        compiler_params=pltpu.CompilerParams(
            collective_id=0, has_side_effects=True, vmem_limit_bytes=VMEM_STEP
        ),
        name="step",
    )(
        *(
            pltpu.with_memory_space_constraint(a, pltpu.HBM)
            for a in (
                gradients.reshape(whole), momentum, worker_error.reshape(whole), server_error, params, variance
            )
        )
    )

    params_next, momentum_next, worker_next, server_next = pl.pallas_call(
        update_kernel,
        out_shape=(
            jax.ShapeDtypeStruct(whole, F32),
            jax.ShapeDtypeStruct(whole, BF16),
            jax.ShapeDtypeStruct(whole, BF16),
            jax.ShapeDtypeStruct(own, BF16),
        ),
        in_specs=[vmem] * 5,
        out_specs=(hbm,) * 4,
        scratch_shapes=[pltpu.VMEM(whole, F32), pltpu.VMEM(whole, BF16), dma((4,))],
        compiler_params=pltpu.CompilerParams(vmem_limit_bytes=VMEM_UPDATE),
        name="update",
    )(
        *(
            pltpu.with_memory_space_constraint(a, pltpu.VMEM)
            for a in (gathered, worker_next, server_next, rate, held)
        )
    )
    return (params_next, momentum_next, worker_next.reshape(1, ROWS, COLS), server_next)


def solution(mesh):
    split = Mesh(mesh.devices.reshape(4, 4, 4, 2), DP)
    in_specs = (P(DP, None, None), P(), P(DP, None, None), P(DP, None), P(), P())
    out_specs = (P(), P(), P(DP, None, None), P(DP, None))
    return jax.shard_map(local, mesh=split, in_specs=in_specs, out_specs=out_specs, check_vma=False)
```

```python
import jax
import jax.numpy as jnp
from jax import lax
from jax.experimental import pallas as pl
from jax.experimental.pallas import tpu as pltpu
from jax.sharding import Mesh
from jax.sharding import PartitionSpec as P

MESH = pl.DeviceIdType.MESH
F32, BF16 = jnp.float32, jnp.bfloat16
DP = ("dp_0", "dp_1", "dp_2", "dp_3")
ORDERS = ((0, 1, 2), (1, 2, 0), (2, 0, 1))
ROWS, COLS, N_DEV = 256, 5120, 128
LANES = 128
W = 7 * LANES
WIDTHS = (W, W, W, W, W, COLS - 5 * W)
N_BLOCK = (ROWS // N_DEV) * COLS
CHUNK = 64
VMEM_STEP, VMEM_UPDATE = 26 * 2**20, 9 * 2**20


def lane_tile(start):
    return pl.ds(pl.multiple_of(start, LANES), LANES)


def swap_granules(tiles):
    low = lax.broadcasted_iota(jnp.int32, (8, LANES), 0) < 4
    swapped = []
    for i in range(4):
        pairs = []
        for first, second in ((tiles[0], tiles[1]), (tiles[2], tiles[3])):
            a, b = first[i // 2], second[i // 2]
            if i % 2 == 0:
                pairs.append(jnp.where(low, a, pltpu.roll(b, 4, 0)))
            else:
                pairs.append(jnp.where(low, pltpu.roll(a, 4, 0), b))
        swapped.append(pairs)
    return swapped


def step_kernel(
    g_hbm, m_hbm, e_hbm, se_hbm, p_hbm, v_hbm, m, sn, wn, rate, pv,
    gme, vv, se, comb, scale, o, ra, rb1, rb2, sb2, s1, r2, st, s2, r3, sv, mb, rq,
    in_sem, aux_sem, send_sem, ra_sem, rb1_sem, rb2_sem, r2_sem, r3_sem, rq_sem, q3_sem, d_sem,
):
    pos = [lax.axis_index(DP[a]) for a in range(3)]
    c = lax.axis_index(DP[3])
    other = 1 - c

    def step(v, d):
        return lax.rem(v + d, 4)

    def device(axis, delta, core):
        at = list(pos)
        if not isinstance(delta, int) or delta:
            at[axis] = step(pos[axis], delta)
        return (*at, core)

    def push(stage, src, dst, sem, to):
        pltpu.make_async_remote_copy(
            src_ref=src, dst_ref=dst, send_sem=send_sem.at[stage], recv_sem=sem,
            device_id=to, device_id_type=MESH,
        ).start()

    def left(stage, alike):
        pltpu.make_async_remote_copy(
            src_ref=alike, dst_ref=alike, send_sem=send_sem.at[stage], recv_sem=d_sem.at[0],
            device_id=device(0, 0, other), device_id_type=MESH,
        ).wait_send()

    def arrived(dst, sem):
        pltpu.make_async_remote_copy(
            src_ref=dst, dst_ref=dst, send_sem=send_sem.at[0], recv_sem=sem,
            device_id=device(0, 0, other), device_id_type=MESH,
        ).wait_recv()

    barrier = pltpu.get_barrier_semaphore()
    for i in range(ROWS // CHUNK):
        rows = pl.ds(i * CHUNK, CHUNK)
        for n, src in enumerate((g_hbm, m_hbm, e_hbm)):
            pltpu.make_async_copy(src.at[rows], gme.at[n, rows], in_sem.at[i]).start()

    peers = [(*pos, other)]
    for x in range(4):
        for z in range(4):
            for y in range(4):
                if x * z * y == 0 and x + z + y > 0:
                    chip = (step(pos[0], x), step(pos[1], z), step(pos[2], y))
                    peers += [(*chip, 0), (*chip, 1)]
    for peer in peers:
        pl.semaphore_signal(barrier, inc=1, device_id=peer, device_id_type=MESH)

    even = lax.broadcasted_iota(jnp.int32, (8, LANES), 0) % 2 == 0
    for i in range(ROWS // CHUNK):
        rows = pl.ds(i * CHUNK, CHUNK)
        pltpu.make_async_copy(gme.at[:, rows], gme.at[:, rows], in_sem.at[i]).wait()

        def square(t, acc, rows=rows):
            cols = lane_tile(t * LANES)
            value = (
                0.875 * gme[1, rows, cols].astype(F32)
                + 0.125 * gme[0, rows, cols].astype(F32)
                + gme[2, rows, cols].astype(F32)
            )
            comb[rows, cols] = value
            return acc + value * value

        acc = lax.fori_loop(0, COLS // LANES, square, jnp.zeros((CHUNK, LANES), F32), unroll=8)
        for s in range(CHUNK // 8):
            row = jnp.sum(acc[8 * s : 8 * s + 8], axis=1, keepdims=True)
            row = jnp.broadcast_to(row, (8, LANES))
            both = row + jnp.where(even, pltpu.roll(row, 7, 0), pltpu.roll(row, 1, 0))
            rounded = jnp.sqrt(both * (1.0 / N_BLOCK)).astype(BF16)
            scale[pl.ds(i * CHUNK + 8 * s, 8)] = rounded.astype(F32)

    se_copy = pltpu.make_async_copy(se_hbm, se, aux_sem.at[0])
    v_copy = pltpu.make_async_copy(v_hbm, vv, aux_sem.at[1])
    p_copy = pltpu.make_async_copy(p_hbm, pv, aux_sem.at[2])
    for copy in (se_copy, v_copy, p_copy):
        copy.start()
    pl.semaphore_wait(barrier, len(peers))

    partner = device(0, 0, other)
    ring = [tuple(step(pos[order[0]], d) for d in range(4)) for order in ORDERS]

    for h in range(2):
        for k, order in enumerate(ORDERS):
            piece = 2 * k + h

            def column(j, carry, piece=piece, k=k, h=h):
                src, dst = lane_tile(piece * W + j * LANES), lane_tile(j * LANES)
                for outer in range(4):
                    tiles = []
                    for inner in range(4):
                        x, z = (inner, outer) if k == 1 else (outer, inner)
                        parts = []
                        for s in range(2):
                            rows = pl.ds(16 * (4 * x + z) + 8 * s, 8)
                            size = scale[rows]
                            parts.append(jnp.where(comb[rows, src] >= 0, size, -size))
                        tiles.append(parts)
                    if k != 0:
                        tiles = swap_granules(tiles)
                    for i in range(4):
                        far, near = (i, outer) if k == 2 else (outer, i)
                        half, row = 2 * far + near // 2, (near % 2) * 16
                        o[k, h, half, pl.ds(row, 16), dst] = jnp.concatenate(tiles[i], 0).astype(BF16)
                return carry

            lax.fori_loop(0, WIDTHS[piece] // LANES, column, 0)
            if WIDTHS[piece] < W:
                spare = W - WIDTHS[piece]
                for half in range(8):
                    o[k, h, half, :, pl.ds(WIDTHS[piece], spare)] = jnp.zeros((32, spare), BF16)
            p2 = ring[k][2]
            push(0, o.at[k, h, 2 * p2], ra.at[k, 0, c], ra_sem.at[k, 0], device(order[0], 1, h))
            push(0, o.at[k, h, 2 * p2 + 1], ra.at[k, 1, c], ra_sem.at[k, 1], device(order[0], 3, h))
    for k, order in enumerate(ORDERS):
        p, p1, _, p3 = ring[k]
        push(0, o.at[k, other, 2 * p1], ra.at[k, 0, 2], ra_sem.at[k, 0], partner)
        push(0, o.at[k, other, 2 * p3 + 1], ra.at[k, 1, 2], ra_sem.at[k, 1], partner)
    for k, order in enumerate(ORDERS):
        p, p1, _, p3 = ring[k]
        for h in range(2):
            push(1, o.at[k, h, 2 * p1 + 1], rb1.at[k, c], rb1_sem.at[k], device(order[0], 1, h))
            push(1, o.at[k, h, 2 * p3], rb1.at[k, 2 + c], rb1_sem.at[k], device(order[0], 3, h))
    for k in range(3):
        push(1, o.at[k, other, pl.ds(2 * ring[k][0], 2)], rb1.at[k, pl.ds(4, 2)], rb1_sem.at[k], partner)

    def rest_column(j, carry):
        cols = lane_tile(j * LANES)
        for top in range(0, ROWS, 16):
            rows = pl.ds(top, 16)
            value, size = comb[rows, cols], scale[rows]
            wn[rows, cols] = (value - jnp.where(value >= 0, size, -size)).astype(BF16)
        return carry

    lax.fori_loop(0, COLS // LANES, rest_column, 0)

    for half in range(2):
        rows = pl.ds(16 * half, 16)
        for k, order in enumerate(ORDERS):
            p, p1, _, p3 = ring[k]
            for d in range(2):
                if half == 0:
                    arrived(ra.at[k, d], ra_sem.at[k, d])
                sb2[k, d, rows] = (
                    (o[k, c, 2 * p1 if d == 0 else 2 * p3 + 1, rows].astype(F32) + ra[k, d, 2, rows].astype(F32))
                    + (ra[k, d, 0, rows].astype(F32) + ra[k, d, 1, rows].astype(F32))
                )
                to = device(order[0], 1 if d == 0 else 3, c)
                push(2, sb2.at[k, d, rows], rb2.at[k, d, rows], rb2_sem.at[k, half], to)

    for half in range(2):
        rows = pl.ds(16 * half, 16)
        for k, order in enumerate(ORDERS):
            p, q = ring[k][0], pos[order[1]]
            if half == 0:
                arrived(rb1.at[k], rb1_sem.at[k])
            arrived(rb2.at[k, 0], rb2_sem.at[k, half])
            for d in range(2):
                s1[k, 2 * d + half] = (
                    (o[k, c, 2 * p + d, rows].astype(F32) + rb1[k, 4 + d, rows].astype(F32))
                    + (rb1[k, 2 - 2 * d, rows].astype(F32) + rb1[k, 3 - 2 * d, rows].astype(F32))
                    + rb2[k, d, rows]
                )
            for to in (half, 2 + half):

                @pl.when(q != to)
                def _(k=k, order=order, q=q, to=to):
                    delta = step(to + 4, -q)
                    push(3, s1.at[k, to], r2.at[k, delta - 1], r2_sem.at[k], device(order[1], delta, c))

    def rate_column(j, carry):
        cols = lane_tile(j * LANES)
        for top in range(0, ROWS, 16):
            rows = pl.ds(top, 16)
            rate[rows, cols] = 0.5 / (jnp.sqrt(vv[rows, cols].astype(F32)) + 1e-08)
        return carry

    v_copy.wait()

    for k, order in enumerate(ORDERS):
        q, r = pos[order[1]], pos[order[2]]
        arrived(r2.at[k], r2_sem.at[k])
        st[k] = (s1[k, q] + r2[k, 0]) + (r2[k, 1] + r2[k, 2])
        for i in range(8):
            s2[k, i] = st[k, pl.ds(2 * i, 2), :]
        for delta in (2, 1, 3):
            for core in range(2):
                src, dst = s2.at[k, 2 * step(r, delta) + core], r3.at[k, 2 * delta + c]
                push(4, src, dst, r3_sem.at[k], device(order[2], delta, core))
        push(4, s2.at[k, 2 * r + other], r3.at[k, c], r3_sem.at[k], partner)
        r3[k, c] = s2[k, 2 * r + c]

    se_copy.wait()
    squares = jnp.zeros((2, LANES), F32)
    for piece in range(6):
        k, h = divmod(piece, 2)
        if h == 0:
            arrived(r3.at[k, pl.ds(0, 7)], r3_sem.at[k])
        width = WIDTHS[piece]
        cols = pl.ds(0, width)
        total = (r3[k, h, :, cols] + r3[k, 2 + h, :, cols]) + (r3[k, 4 + h, :, cols] + r3[k, 6 + h, :, cols])
        served = total * (1.0 / N_DEV) + se[:, pl.ds(piece * W, width)].astype(F32)
        sv[piece, :, cols] = served
        for t in range(width // LANES):
            part = served[:, t * LANES : (t + 1) * LANES]
            squares = squares + part * part
    total = jnp.sum(jnp.sum(squares, axis=1, keepdims=True), axis=0, keepdims=True)
    size = jnp.sqrt(total * (1.0 / N_BLOCK)).astype(BF16).astype(F32)
    for piece in range(6):
        k, h = divmod(piece, 2)
        width = WIDTHS[piece]
        cols = pl.ds(0, width)
        served = sv[piece, :, cols]
        level = jnp.broadcast_to(size, (2, width))
        comp = jnp.where(served >= 0, level, -level)
        sn[:, pl.ds(piece * W, width)] = (served - comp).astype(BF16)
        mb[k, h, :, cols] = comp.astype(BF16)
        if width < W:
            mb[k, h, :, pl.ds(width, W - width)] = jnp.zeros((2, W - width), BF16)

    def place(k, q_shift, r_shift, core):
        at = list(pos)
        at[ORDERS[k][1]] = step(at[ORDERS[k][1]], q_shift)
        at[ORDERS[k][2]] = step(at[ORDERS[k][2]], r_shift)
        return (*at, core)

    for q_shift in (0, 1, 3, 2):
        for r_shift in (2, 1, 3, 0):
            for k, order in enumerate(ORDERS):
                q, mine = pos[order[1]], 2 * pos[order[2]] + c
                sem = rq_sem.at[k, (0, 1, 2, 1)[q_shift]]
                if q_shift or r_shift:
                    for h in range(2):
                        push(8 if q_shift else 5, mb.at[k, h], rq.at[k, q, mine], sem, place(k, q_shift, r_shift, h))
                else:
                    push(5, mb.at[k, other], rq.at[k, q, mine], sem, partner)
                    rq[k, q, mine] = mb[k, c]

    def spread(k, at, group):
        order = ORDERS[k]
        view = m.at[k, c, ring[k][0], at]
        for delta in (2, 1, 3):
            push(6, view, view, q3_sem.at[k, group], device(order[0], delta, c))
        push(7, view, view, d_sem.at[0], partner)

    lax.fori_loop(0, COLS // LANES, rate_column, 0)
    for group, shifts in enumerate(((0,), (1, 3), (2,))):
        for k, order in enumerate(ORDERS):
            q = pos[order[1]]
            arrived(rq.at[k, 0, pl.ds(0, 7)] if group == 0 else rq.at[k, pl.ds(0, len(shifts))], rq_sem.at[k, group])
            for shift in shifts:
                at = step(q, shift)
                for i in range(8):
                    st[k, pl.ds(2 * i, 2), :] = rq[k, at, i].astype(F32)
                m[k, c, pos[order[0]], at] = st[k].astype(BF16)
            for shift in shifts:
                spread(k, step(q, shift), group)
    for group, tiles in enumerate(((0,), (1, 3), (2,))):
        for k, order in enumerate(ORDERS):
            arrived(m.at[k, 0, pl.ds(0, 3), pl.ds(0, len(tiles))], q3_sem.at[k, group])
            for delta in (1, 3, 2):
                at, q = step(pos[order[0]], 4 - delta), pos[order[1]]
                for shift in tiles:
                    view = m.at[k, c, at, step(q, shift)]
                    push(7, view, view, d_sem.at[0], partner)
    arrived(m.at[:, other], d_sem.at[0])
    p_copy.wait()
    for stage, alike in enumerate((
        ra, rb1, rb2, r2, r3.at[:, pl.ds(0, 7)], rq.at[:, 0, pl.ds(0, 7)],
        m.at[:, 0, pl.ds(0, 3)], m.at[:, 0], rq.at[:, pl.ds(0, 3)],
    )):
        left(stage, alike)


def update_kernel(m, wn, sn, rate, pv, params_next, momentum_next, worker_next, server_next, pn, mn, sem):
    whole = [
        pltpu.make_async_copy(wn, worker_next, sem.at[0]),
        pltpu.make_async_copy(sn, server_next, sem.at[1]),
    ]
    for copy in whole:
        copy.start()
    for piece in range(6):
        k, h = divmod(piece, 2)

        def column(j, carry, piece=piece, k=k, h=h):
            src, dst = lane_tile(j * LANES), lane_tile(piece * W + j * LANES)
            for outer in range(4):
                tiles = []
                for i in range(4):
                    far, near = (i, outer) if k == 2 else (outer, i)
                    tile = m[k, h, far, near, :, src].astype(F32)
                    tiles.append([tile[:8], tile[8:]])
                if k != 0:
                    tiles = swap_granules(tiles)
                for inner in range(4):
                    x, z = (inner, outer) if k == 1 else (outer, inner)
                    rows = pl.ds(16 * (4 * x + z), 16)
                    value = jnp.concatenate(tiles[inner], 0)
                    mn[rows, dst] = value.astype(BF16)
                    pn[rows, dst] = pv[rows, dst] - value * rate[rows, dst]
            return carry

        lax.fori_loop(0, WIDTHS[piece] // LANES, column, 0)
        cols = pl.ds(piece * W, WIDTHS[piece])
        pltpu.make_async_copy(pn.at[:, cols], params_next.at[:, cols], sem.at[2]).start()
        pltpu.make_async_copy(mn.at[:, cols], momentum_next.at[:, cols], sem.at[3]).start()
    whole += [
        pltpu.make_async_copy(pn, params_next, sem.at[2]),
        pltpu.make_async_copy(mn, momentum_next, sem.at[3]),
    ]
    for copy in whole:
        copy.wait()


def local(gradients, momentum, worker_error, server_error, params, variance):
    hbm = pl.BlockSpec(memory_space=pltpu.HBM)
    vmem = pl.BlockSpec(memory_space=pltpu.VMEM)
    dma = pltpu.SemaphoreType.DMA
    whole = (ROWS, COLS)
    own = (ROWS // N_DEV, COLS)
    gathered, server_next, worker_next, rate, held = pl.pallas_call(
        step_kernel,
        out_shape=(
            pltpu.VMEM((3, 2, 4, 4, 16, W), BF16),
            pltpu.VMEM(own, BF16),
            pltpu.VMEM(whole, BF16),
            pltpu.VMEM(whole, F32),
            pltpu.VMEM(whole, F32),
        ),
        in_specs=[hbm] * 6,
        out_specs=(vmem,) * 5,
        scratch_shapes=[
            pltpu.VMEM((3, ROWS, COLS), BF16),
            pltpu.VMEM(whole, BF16),
            pltpu.VMEM(own, BF16),
            pltpu.VMEM(whole, F32),
            pltpu.VMEM((ROWS, LANES), F32),
            pltpu.VMEM((3, 2, 8, 32, W), BF16),
            pltpu.VMEM((3, 2, 3, 32, W), BF16),
            pltpu.VMEM((3, 6, 32, W), BF16),
            pltpu.VMEM((3, 2, 32, W), F32),
            pltpu.VMEM((3, 2, 32, W), F32),
            pltpu.VMEM((3, 4, 16, W), F32),
            pltpu.VMEM((3, 3, 16, W), F32),
            pltpu.VMEM((3, 16, W), F32),
            pltpu.VMEM((3, 8, 2, W), F32),
            pltpu.VMEM((3, 8, 2, W), F32),
            pltpu.VMEM((6, 2, W), F32),
            pltpu.VMEM((3, 2, 2, W), BF16),
            pltpu.VMEM((3, 4, 8, 2, W), BF16),
            dma((ROWS // CHUNK,)),
            dma((3,)),
            dma((9,)),
            dma((3, 2)),
            dma((3,)),
            dma((3, 2)),
            dma((3,)),
            dma((3,)),
            dma((3, 3)),
            dma((3, 3)),
            dma((1,)),
        ],
        compiler_params=pltpu.CompilerParams(
            collective_id=0, has_side_effects=True, vmem_limit_bytes=VMEM_STEP
        ),
        name="step",
    )(
        *(
            pltpu.with_memory_space_constraint(a, pltpu.HBM)
            for a in (
                gradients.reshape(whole), momentum, worker_error.reshape(whole), server_error, params, variance
            )
        )
    )

    params_next, momentum_next, worker_next, server_next = pl.pallas_call(
        update_kernel,
        out_shape=(
            jax.ShapeDtypeStruct(whole, F32),
            jax.ShapeDtypeStruct(whole, BF16),
            jax.ShapeDtypeStruct(whole, BF16),
            jax.ShapeDtypeStruct(own, BF16),
        ),
        in_specs=[vmem] * 5,
        out_specs=(hbm,) * 4,
        scratch_shapes=[pltpu.VMEM(whole, F32), pltpu.VMEM(whole, BF16), dma((4,))],
        compiler_params=pltpu.CompilerParams(vmem_limit_bytes=VMEM_UPDATE),
        name="update",
    )(
        *(
            pltpu.with_memory_space_constraint(a, pltpu.VMEM)
            for a in (gathered, worker_next, server_next, rate, held)
        )
    )
    return (params_next, momentum_next, worker_next.reshape(1, ROWS, COLS), server_next)


def solution(mesh):
    split = Mesh(mesh.devices.reshape(4, 4, 4, 2), DP)
    in_specs = (P(DP, None, None), P(), P(DP, None, None), P(DP, None), P(), P())
    out_specs = (P(), P(), P(DP, None, None), P(DP, None))
    return jax.shard_map(local, mesh=split, in_specs=in_specs, out_specs=out_specs, check_vma=False)
```
